512 devices in a mesh: pts: 32 (over y, x), cen: 16 (over z, core).
Axes of the slice: x: 4, y: 8, z: 8, core: 2. Of those that a mesh axis runs over, the one named last changes fastest.
Arguments:
- points: bfloat16 [131072, 1024], P('pts'), may hold values from -60 to 60
- fine_assign: int32 [2, 131072], P(None, 'pts'), may hold values from 0 to 2047
- fine_start: float32 [2048, 1024], P('cen'), may hold values from -3 to 3
- coarse_start: float32 [64, 1024], replicated, may hold values from -3 to 3
- coarse_assign: int32 [2048], P('cen'), may hold values from 0 to 63
Outputs:
- fine_centroids: float32 [2048, 1024], P('cen')
- coarse_centroids: float32 [64, 1024], replicated
- gaps: float32 [2, 131072], P(None, 'pts')
The draws below stay inside these ranges and needn't reach their ends.
All inputs are finite; a program needn't handle non-finite values.
Results may differ from the reference program's by a relative error of at most 0.0028.
Values sent between devices are 32-bit elements; how exact they have to be, the bound alone decides.
A program may use at most 64 MiB of HBM per device.

```python
import math
import jax
import jax.numpy as jnp
from jax import lax

D = 1024
NF = 2048
NC = 64
PASSES = 2
NPTS = 131072


def draw_points(key, part):
    first, second = jax.random.split(jax.random.fold_in(key, 11), 2)
    positions = jnp.arange(NPTS, dtype=jnp.float32) / NPTS
    base = jax.random.truncated_normal(first, -6.0, 6.0, (NPTS, D), jnp.float32)
    rising = jnp.exp(math.log(3.0) * positions)
    scales = jnp.exp(jax.random.uniform(second, (NPTS,), jnp.float32, math.log(0.3), math.log(3.0))) * rising
    return (base * scales[:, None]).astype(jnp.bfloat16)


def with_ends(result, own_key, smallest, top_value):
    longest = result.shape.index(max(result.shape))
    spots = []
    for shift in (0, 1):
        where = [jax.random.randint(jax.random.fold_in(own_key, axis), (), 0, length) for axis, length in enumerate(result.shape)]
        where[longest] = (where[longest] + shift) % result.shape[longest]
        spots.append(tuple(where))
    return result.at[spots[0]].set(smallest).at[spots[1]].set(top_value)


def level_of(own_key, dims, cuts, smallest, largest):
    def one(axis_at, parts):
        heights = jax.random.uniform(jax.random.fold_in(jax.random.fold_in(own_key, 6), axis_at), (parts,), jnp.float32, smallest / len(cuts), largest / len(cuts))
        return jnp.repeat(jnp.exp(heights), dims[axis_at] // parts).reshape((-1,) + (1,) * (len(dims) - axis_at - 1))

    loudness = one(*cuts[0])
    for cut in cuts[1:]:
        loudness = loudness * one(*cut)
    return loudness


def scatter_about(rng, extent, scale, bound, pieces=(), kind=jnp.bfloat16):
    factor_of = level_of(rng, extent, pieces, -0.22, 0.18) if pieces else 1.0
    drawn = jax.random.normal(rng, extent, jnp.float32) * scale * factor_of
    return jnp.minimum(jnp.maximum(drawn, -bound), bound).astype(kind)


def setup_inputs(seed: int = 0) -> dict:
    streams_of = jax.random.split(jax.random.key(seed), 6)
    return {
        "points": draw_points(jax.random.fold_in(streams_of[5], 71), 0),
        "fine_assign": with_ends(jax.random.randint(streams_of[1], (PASSES, NPTS), 0, NF), jax.random.fold_in(streams_of[1], 1), 0, NF - 1).astype(jnp.int32),
        "fine_start": scatter_about(streams_of[2], (NF, D), 0.5, 3.0, ((0, 16),), jnp.float32),
        "coarse_start": scatter_about(streams_of[3], (NC, D), 0.5, 3.0, (), jnp.float32),
        "coarse_assign": with_ends(jax.random.randint(streams_of[4], (NF,), 0, NC), jax.random.fold_in(streams_of[4], 1), 0, NC - 1).astype(jnp.int32),
    }


prior_weight = 4.0

def reference(points, fine_assign, fine_start, coarse_start, coarse_assign):
    block = math.gcd(NPTS, 512)
    blocks = NPTS // block
    point_values = points.astype(jnp.float32)
    squares = lax.optimization_barrier(jnp.sum(point_values * point_values, axis=1))
    fine = fine_start
    coarse = coarse_start
    gap_rows = []
    for pass_index in range(PASSES):
        assign = fine_assign[pass_index]
        fine_low = fine.astype(jnp.bfloat16).astype(jnp.float32)
        norms = lax.optimization_barrier(jnp.sum(fine * fine, axis=1))

        def block_terms(items):
            rows_in, ids_in = items
            products = jnp.dot(rows_in.astype(jnp.float32), fine_low.T, precision=lax.Precision.HIGHEST)
            energy = norms[None, :] - 2.0 * products
            picked_one = jnp.take_along_axis(energy, ids_in[:, None].astype(jnp.int32), axis=1)[:, 0]
            return (picked_one, lax.optimization_barrier(jnp.min(energy, axis=1)))
        picked, nearest = lax.map(block_terms, (points.reshape(blocks, block, D), assign.reshape(blocks, block)))
        picked = picked.reshape(NPTS)
        nearest = nearest.reshape(NPTS)
        gap_rows.append((picked - nearest) / math.sqrt(D))
        weights = 1.0 / (1.0 + (squares + picked) / D)
        scaled = (point_values * weights[:, None]).astype(jnp.bfloat16)
        totals = jax.ops.segment_sum(scaled.astype(jnp.float32), assign, NF)
        counts = jax.ops.segment_sum(weights, assign, NF)
        lookup = coarse[coarse_assign]
        fine = (totals + prior_weight * lookup) / (counts + prior_weight)[:, None]
        coarse_sum = jax.ops.segment_sum(counts[:, None] * fine, coarse_assign, NC)
        coarse_count = jax.ops.segment_sum(counts, coarse_assign, NC)
        coarse = (coarse_sum + prior_weight * coarse) / (coarse_count + prior_weight)[:, None]
    return (fine, coarse, jnp.stack(gap_rows))
```

```python
import jax
import jax.numpy as jnp
from jax import lax
from jax.experimental import pallas as pl
from jax.experimental.pallas import tpu as pltpu
from jax.sharding import PartitionSpec as P

NC = 64
PASSES = 2
PRIOR = 4.0
D = 1024
NP = 4096
NK = 128
NX, NY, NCEN = 4, 8, 16
CH = 512
STEPS = NP // CH
GP = NP // NCEN
F32 = jnp.float32
BF16 = jnp.bfloat16
MESH = pl.DeviceIdType.MESH
HIGH = lax.Precision.HIGHEST

FIRST = 8 + 128
ROWS = FIRST + 128


def dot_nt(a, b):
    return lax.dot_general(a, b, (((1,), (1,)), ((), ())), precision=HIGH, preferred_element_type=F32)


def kernel(
    points, assign, fine_start, coarse_start, coarse_assign,
    fine_out, coarse_out, gaps_out,
    xv, av, fv, cv, kv, in_sem,
    low, norm, squares, wv, cacc,
    ahead, hop_r, hop_l, blk_r, blk_l, got_l, got_r, ysend, yrecv,
    fine_g, cpack, crecv, coarse_g,
    pn, pn_recv, gap_g,
    rs_s, rs_r, ys_s, ys_r, gy_s, gy_r, gx_s, gx_r, cs_s, cs_r, cy_s, cy_r, cx_s, cx_r, p_s, p_r, g_s, g_r,
):
    pts = lax.axis_index("pts")
    cen = lax.axis_index("cen")
    y = pts // NX
    x = pts % NX
    x_right, x_left, x_far = (x + 1) % NX, (x + 3) % NX, (x + 2) % NX
    right = {"pts": y * NX + x_right}
    left = {"pts": y * NX + x_left}

    def y_peer(d):
        return {"pts": ((y + d) % NY) * NX + x}

    def c_peer(d):
        return {"cen": (cen + d) % NCEN}

    sends = []

    def remote(src, dst, s, r, where):
        copy = pltpu.make_async_remote_copy(
            src_ref=src, dst_ref=dst, send_sem=s, recv_sem=r, device_id=where, device_id_type=MESH
        )
        copy.start()
        sends.append(copy)
        return copy

    fine_in = pltpu.make_async_copy(fine_start, fv, in_sem.at[STEPS])
    fine_in.start()

    def x_copy(i):
        rows = pl.ds(pl.multiple_of(i * CH, CH), CH)
        return pltpu.make_async_copy(points.at[rows], xv.at[rows], in_sem.at[i])

    for i in range(STEPS):
        x_copy(i).start()
    a_in = pltpu.make_async_copy(assign, av, in_sem.at[STEPS + 1])
    k_in = pltpu.make_async_copy(coarse_assign, kv, in_sem.at[STEPS + 2])
    c_in = pltpu.make_async_copy(coarse_start, cv, in_sem.at[STEPS + 3])
    a_in.start()
    k_in.start()
    c_in.start()

    barrier = pltpu.get_barrier_semaphore()
    for where in [right, left] + [y_peer(d) for d in range(1, NY)] + [c_peer(d) for d in range(1, NCEN)]:
        pl.semaphore_signal(barrier, inc=1, device_id=where, device_id_type=MESH)

    fine_in.wait()
    total = jnp.zeros((1, NK), F32)
    for b in range(D // 128):
        t = fv[:, b * 128 : (b + 1) * 128].T
        low[b * 128 : (b + 1) * 128, :] = t.astype(BF16)
        total = total + jnp.sum(t * t, axis=0, keepdims=True)
    norm[...] = total
    a_in.wait()
    k_in.wait()
    c_in.wait()

    own = lax.broadcasted_iota(jnp.int32, (NK, CH), 0) + cen * NK

    def energies(p):
        cacc[...] = jnp.zeros_like(cacc)

        def body(i, carry):
            if p == 0:
                x_copy(i).wait()
            rows = pl.ds(pl.multiple_of(i * CH, CH), CH)
            xs = xv[rows, :]
            products = jnp.dot(xs, low[...], preferred_element_type=F32)
            energy = (norm[...] - 2.0 * products).T
            if p == 0:
                part = jnp.zeros((CH, 128), F32)
                for g in range(D // 128):
                    xf = xs[:, g * 128 : (g + 1) * 128].astype(F32)
                    part = part + xf * xf
                sq = jnp.sum(part.T, axis=0, keepdims=True)
                squares[i] = sq
            else:
                sq = squares[i]
            member = av[p : p + 1, rows] == own
            picked = jnp.sum(jnp.where(member, energy, 0.0), axis=0, keepdims=True)
            nearest = jnp.min(energy, axis=0, keepdims=True)
            weights = 1.0 / (1.0 + (sq + picked) / D)
            wm = jnp.where(member, weights, 0.0)
            high = wm.astype(BF16)
            wv[0:NK, rows] = high
            wv[NK : 2 * NK, rows] = (wm - high.astype(F32)).astype(BF16)
            for g in range(CH // 128):
                cacc[...] += wm[:, g * 128 : (g + 1) * 128]
            for g in range(CH // GP):
                pn[i * (CH // GP) + g, 2 * p : 2 * p + 1, :] = picked[:, g * GP : (g + 1) * GP]
                pn[i * (CH // GP) + g, 2 * p + 1 : 2 * p + 2, :] = nearest[:, g * GP : (g + 1) * GP]
            return carry

        lax.fori_loop(0, STEPS, body, 0)

    def block(b):
        cols = pl.multiple_of(b * 128, 128)
        rhs = jnp.concatenate([xv[:, pl.ds(cols, 128)], xv[:, pl.ds(512 + cols, 128)]], axis=1)
        both = jnp.dot(wv[...], rhs, preferred_element_type=F32)
        return (both[:NK] + both[NK:]).T

    share = x * NY + y
    turned = jnp.concatenate([cv[:, 0:512], cv[:, 512:1024]], axis=0).T
    cpack[...] = turned
    of = lax.broadcasted_iota(jnp.int32, (128, NK), 0)
    pick_a = (of == kv[...]).astype(F32)
    pick_b = (of == kv[...] + NC).astype(F32)
    coarse = cpack[pl.ds(pl.multiple_of(share * 16, 16), 16), :]

    pl.semaphore_wait(barrier, 2 + (NY - 1) + (NCEN - 1))

    for p in range(PASSES):
        last = p == PASSES - 1
        energies(p)
        if last:
            pn_copies = [
                remote(pn.at[(cen + d) % NCEN], pn_recv.at[d], p_s.at[d], p_r.at[d], c_peer(d))
                for d in range(1, NCEN)
            ]
        counts8 = jnp.sum(cacc[...].T.reshape(16, 8, NK), axis=0)

        t = block(x_far)
        ahead[p, 0:8, :] = counts8
        ahead[p, 8:ROWS, :] = t
        h1 = remote(ahead.at[p, 0:FIRST], hop_r.at[p], rs_s.at[p, 0], rs_r.at[p, 0], right)
        h2 = remote(ahead.at[p, FIRST:ROWS], hop_l.at[p], rs_s.at[p, 1], rs_r.at[p, 1], left)
        t = block(x_right)
        blk_r[p, FIRST:ROWS, :] = t[128:]
        r2 = remote(
            blk_r.at[p, FIRST:ROWS], got_l.at[p, FIRST:ROWS], rs_s.at[p, 2], rs_r.at[p, 2], right
        )
        blk_r[p, 0:8, :] = counts8
        blk_r[p, 8:FIRST, :] = t[:128]
        t = block(x_left)
        blk_l[p, 0:8, :] = counts8
        blk_l[p, 8:FIRST, :] = t[:128]
        l1 = remote(blk_l.at[p, 0:FIRST], got_r.at[p, 0:FIRST], rs_s.at[p, 3], rs_r.at[p, 3], left)
        h1.wait_recv()
        blk_r[p, 0:FIRST, :] += hop_r[p]
        r1 = remote(blk_r.at[p, 0:FIRST], got_l.at[p, 0:FIRST], rs_s.at[p, 4], rs_r.at[p, 4], right)
        h2.wait_recv()
        blk_l[p, FIRST:ROWS, :] = t[128:] + hop_l[p]
        l2 = remote(
            blk_l.at[p, FIRST:ROWS], got_r.at[p, FIRST:ROWS], rs_s.at[p, 5], rs_r.at[p, 5], left
        )
        t = block(x)
        for copy in (r2, l1, r1, l2):
            copy.wait_recv()
        counts8 = counts8 + got_l[p, 0:8, :] + got_r[p, 0:8, :]
        t = t + got_l[p, 8:ROWS, :] + got_r[p, 8:ROWS, :]
        for k in range(NY):
            ysend[p, k, 0:16, :] = t[k * 16 : (k + 1) * 16]
            ysend[p, k, 16:32, :] = t[128 + k * 16 : 128 + (k + 1) * 16]
            ysend[p, k, 32:40, :] = counts8
        ycopies = [
            remote(ysend.at[p, (y + d) % NY], yrecv.at[p, d], ys_s.at[p, d], ys_r.at[p, d], y_peer(d))
            for d in range(1, NY)
        ]
        if p > 0:
            coarse = coarse_update(ccopies, crecv, p - 1, coarse)
        lookup = jnp.concatenate(
            [
                jnp.dot(coarse, pick_a, precision=HIGH, preferred_element_type=F32),
                jnp.dot(coarse, pick_b, precision=HIGH, preferred_element_type=F32),
            ],
            axis=0,
        )
        if last:
            finish = pn[cen]
            picked0, near0, picked1, near1 = (finish[k : k + 1] for k in range(4))
            for d in range(1, NCEN):
                pn_copies[d - 1].wait_recv()
                picked0 = picked0 + pn_recv[d, 0:1, :]
                near0 = jnp.minimum(near0, pn_recv[d, 1:2, :])
                picked1 = picked1 + pn_recv[d, 2:3, :]
                near1 = jnp.minimum(near1, pn_recv[d, 3:4, :])
            gap_g[cen, 0:1, :] = (picked0 - near0) / 32.0
            gap_g[cen, 1:2, :] = (picked1 - near1) / 32.0
            gap_copies = [
                remote(gap_g.at[cen], gap_g.at[cen], g_s.at[d], g_r.at[d], c_peer(d)) for d in range(1, NCEN)
            ]
        all_sum = ysend[p, y]
        for d in range(1, NY):
            ycopies[d - 1].wait_recv()
            all_sum = all_sum + yrecv[p, d]
        counts = jnp.sum(all_sum[32:40], axis=0, keepdims=True)
        fine = (all_sum[0:32] + PRIOR * lookup) / (counts + PRIOR)
        fine_g[p, x, y] = fine
        gy = [
            remote(fine_g.at[p, x, y], fine_g.at[p, x, y], gy_s.at[p, d], gy_r.at[p, d], y_peer(d))
            for d in range(1, NY)
        ]
        weighted = counts * fine
        crecv[p, cen, 0:16, :] = dot_nt(weighted[0:16], pick_a) + dot_nt(weighted[16:32], pick_b)
        crecv[p, cen, 16:24, :] = dot_nt(jnp.broadcast_to(counts, (8, NK)), pick_a + pick_b)
        ccopies = [
            remote(crecv.at[p, cen], crecv.at[p, cen], cs_s.at[p, d], cs_r.at[p, d], c_peer(d))
            for d in range(1, NCEN)
        ]
        for copy in gy:
            copy.wait_recv()
        lo, hi = pl.ds(0, NY // 2), pl.ds(NY // 2, NY // 2)

        def to(where, half, sem):
            ref = fine_g.at[p, x, half]
            return remote(ref, ref, gx_s.at[p, sem], gx_r.at[p, sem], where)

        r_lo = to(right, lo, 0)
        l_hi = to(left, hi, 1)
        r_hi = to(right, hi, 2)
        l_lo = to(left, lo, 3)
        if last:
            coarse = coarse_update(ccopies, crecv, p, coarse)
            coarse_g[x, y] = coarse
            cy = [
                remote(coarse_g.at[x, y], coarse_g.at[x, y], cy_s.at[d], cy_r.at[d], y_peer(d))
                for d in range(1, NY)
            ]
        r_lo.wait_recv()
        ref = fine_g.at[p, x_left, lo]
        f_r = remote(ref, ref, gx_s.at[p, 4], gx_r.at[p, 4], right)
        l_hi.wait_recv()
        ref = fine_g.at[p, x_right, hi]
        f_l = remote(ref, ref, gx_s.at[p, 5], gx_r.at[p, 5], left)
        if last:
            for copy in cy:
                copy.wait_recv()

            def coarse_to(where, half, sem):
                ref = coarse_g.at[x, half]
                return remote(ref, ref, cx_s.at[sem], cx_r.at[sem], where)

            cr_lo = coarse_to(right, lo, 0)
            cl_hi = coarse_to(left, hi, 1)
            cr_hi = coarse_to(right, hi, 2)
            cl_lo = coarse_to(left, lo, 3)
            for d in range(1, NCEN):
                gap_copies[d - 1].wait_recv()
            for c in range(NCEN):
                gaps_out[:, c * GP : (c + 1) * GP] = gap_g[c]
        for copy in (r_hi, l_lo, f_r, f_l):
            copy.wait_recv()
        if last:
            cr_lo.wait_recv()
            ref = coarse_g.at[x_left, lo]
            cf_r = remote(ref, ref, cx_s.at[4], cx_r.at[4], right)
            cl_hi.wait_recv()
            ref = coarse_g.at[x_right, hi]
            cf_l = remote(ref, ref, cx_s.at[5], cx_r.at[5], left)
        total = jnp.zeros((1, NK), F32)
        for b in range(D // 128):
            h, bx = divmod(b, NX)
            t = fine_g[p, bx, :, h * 16 : (h + 1) * 16, :].reshape(128, NK)
            if last:
                fine_out[:, b * 128 : (b + 1) * 128] = t.T
            else:
                low[b * 128 : (b + 1) * 128, :] = t.astype(BF16)
                total = total + jnp.sum(t * t, axis=0, keepdims=True)
        if not last:
            norm[...] = total

    for copy in (cr_hi, cl_lo, cf_r, cf_l):
        copy.wait_recv()
    t = coarse_g[...].reshape(512, 128).T
    coarse_out[:, 0:512] = t[0:NC]
    coarse_out[:, 512:1024] = t[NC : 2 * NC]
    for copy in sends:
        copy.wait_send()


def coarse_update(copies, crecv, p, coarse):
    for copy in copies:
        copy.wait_recv()
    total = crecv[p, 0]
    for c in range(1, NCEN):
        total = total + crecv[p, c]
    return (total[0:16] + PRIOR * coarse) / (total[16:17] + PRIOR)


def on_device(points, fine_assign, fine_start, coarse_start, coarse_assign):
    dma = pltpu.SemaphoreType.DMA
    vmem = pltpu.VMEM
    n = PASSES
    scratch = [
        vmem((NP, D), BF16), vmem((PASSES, NP), jnp.int32), vmem((NK, D), F32), vmem((NC, D), F32),
        vmem((1, NK), jnp.int32), dma((STEPS + 4,)),
        vmem((D, NK), BF16), vmem((1, NK), F32), vmem((STEPS, 1, CH), F32), vmem((2 * NK, NP), BF16),
        vmem((NK, 128), F32),
        vmem((n, ROWS, 128), F32), vmem((n, FIRST, 128), F32), vmem((n, 128, 128), F32),
        vmem((n, ROWS, 128), F32), vmem((n, ROWS, 128), F32), vmem((n, ROWS, 128), F32), vmem((n, ROWS, 128), F32),
        vmem((n, NY, 40, 128), F32), vmem((n, NY, 40, 128), F32),
        vmem((n, NX, NY, 32, 128), F32), vmem((512, 128), F32), vmem((n, NCEN, 24, 128), F32),
        vmem((NX, NY, 16, 128), F32),
        vmem((NCEN, 4, GP), F32), vmem((NCEN, 4, GP), F32), vmem((NCEN, 2, GP), F32),
        dma((n, 6)), dma((n, 6)), dma((n, NY)), dma((n, NY)), dma((n, NY)), dma((n, NY)),
        dma((n, 6)), dma((n, 6)), dma((n, NCEN)), dma((n, NCEN)), dma((NY,)), dma((NY,)),
        dma((6,)), dma((6,)), dma((NCEN,)), dma((NCEN,)), dma((NCEN,)), dma((NCEN,)),
    ]
    return tuple(pl.pallas_call(
        kernel,
        out_shape=(
            jax.ShapeDtypeStruct((NK, D), F32),
            jax.ShapeDtypeStruct((NC, D), F32),
            jax.ShapeDtypeStruct((PASSES, NP), F32),
        ),
        in_specs=[pl.BlockSpec(memory_space=pl.ANY)] * 5,
        out_specs=[pl.BlockSpec(memory_space=pltpu.VMEM)] * 3,
        scratch_shapes=scratch,
        compiler_params=pltpu.CompilerParams(
            collective_id=0, has_side_effects=True, vmem_limit_bytes=48 * 1024 * 1024
        ),
    )(points, fine_assign, fine_start, coarse_start, coarse_assign.reshape(1, NK)))


def solution(mesh):
    placed = (P("pts", None), P(None, "pts"), P("cen", None), P(), P("cen"))
    return jax.shard_map(
        on_device,
        mesh=mesh,
        in_specs=placed,
        out_specs=(P("cen", None), P(), P(None, "pts")),
        check_vma=False,
    )
```

```python
import jax
import jax.numpy as jnp
from jax import lax
from jax.experimental import pallas as pl
from jax.experimental.pallas import tpu as pltpu
from jax.sharding import PartitionSpec as P

NC = 64
PASSES = 2
PRIOR = 4.0
D = 1024
NP = 4096
NK = 128
NX, NY, NCEN = 4, 8, 16
CH = 512
STEPS = NP // CH
GP = NP // NCEN
F32 = jnp.float32
BF16 = jnp.bfloat16
MESH = pl.DeviceIdType.MESH
HIGH = lax.Precision.HIGHEST

FIRST = 8 + 128
ROWS = FIRST + 128


def dot_nt(a, b):
    return lax.dot_general(a, b, (((1,), (1,)), ((), ())), precision=HIGH, preferred_element_type=F32)


def kernel(
    points, assign, fine_start, coarse_start, coarse_assign,
    fine_hbm, coarse_hbm, gaps_hbm,
    xv, av, fv, cv, kv, in_sem,
    low, norm, prods, squares, wv, cacc,
    ahead, hop_r, hop_l, blk_r, blk_l, got_l, got_r, ysend, yrecv,
    fine_g, cpack, crecv, coarse_g,
    pn, pn_recv, gap_g, fine_out, coarse_out, gaps_out, out_sem,
    rs_s, rs_r, ys_s, ys_r, gy_s, gy_r, gx_s, gx_r, cs_s, cs_r, cy_s, cy_r, cx_s, cx_r, p_s, p_r, g_s, g_r,
):
    pts = lax.axis_index("pts")
    cen = lax.axis_index("cen")
    y = pts // NX
    x = pts % NX
    x_right, x_left, x_far = (x + 1) % NX, (x + 3) % NX, (x + 2) % NX
    right = {"pts": y * NX + x_right}
    left = {"pts": y * NX + x_left}

    def y_peer(d):
        return {"pts": ((y + d) % NY) * NX + x}

    def c_peer(d):
        return {"cen": (cen + d) % NCEN}

    sends = []

    def arrive(name, *copies):
        with jax.named_scope(name):
            for copy in copies:
                copy.wait_recv()

    def remote(src, dst, s, r, where):
        copy = pltpu.make_async_remote_copy(
            src_ref=src, dst_ref=dst, send_sem=s, recv_sem=r, device_id=where, device_id_type=MESH
        )
        copy.start()
        sends.append(copy)
        return copy

    fine_in = pltpu.make_async_copy(fine_start, fv, in_sem.at[STEPS])
    fine_in.start()

    def x_copy(i):
        rows = pl.ds(pl.multiple_of(i * CH, CH), CH)
        return pltpu.make_async_copy(points.at[rows], xv.at[rows], in_sem.at[i])

    a_in = pltpu.make_async_copy(assign, av, in_sem.at[STEPS + 1])
    k_in = pltpu.make_async_copy(coarse_assign, kv, in_sem.at[STEPS + 2])
    c_in = pltpu.make_async_copy(coarse_start, cv, in_sem.at[STEPS + 3])
    a_in.start()
    k_in.start()
    c_in.start()
    for i in range(STEPS):
        x_copy(i).start()

    barrier = pltpu.get_barrier_semaphore()
    for where in [right, left] + [y_peer(d) for d in range(1, NY)] + [c_peer(d) for d in range(1, NCEN)]:
        pl.semaphore_signal(barrier, inc=1, device_id=where, device_id_type=MESH)

    with jax.named_scope('w_fine_in'):
        fine_in.wait()
    total = jnp.zeros((1, NK), F32)
    for b in range(D // 128):
        t = fv[:, b * 128 : (b + 1) * 128].T
        low[b * 128 : (b + 1) * 128, :] = t.astype(BF16)
        total = total + jnp.sum(t * t, axis=0, keepdims=True)
    norm[...] = total
    with jax.named_scope('w_ins'):
        a_in.wait()
        k_in.wait()
        c_in.wait()

    own = lax.broadcasted_iota(jnp.int32, (NK, CH), 0) + cen * NK

    def energies(p):
        cacc[...] = jnp.zeros_like(cacc)

        def multiply(i):
            if p == 0:
                x_copy(i).wait()
            rows = pl.ds(pl.multiple_of(i * CH, CH), CH)
            prods[i % 2] = jnp.dot(xv[rows, :], low[...], preferred_element_type=F32)

        def select(i):
            rows = pl.ds(pl.multiple_of(i * CH, CH), CH)
            energy = (norm[...] - 2.0 * prods[i % 2]).T
            if p == 0:
                part = jnp.zeros((CH, 128), F32)
                for g in range(D // 128):
                    xf = xv[rows, g * 128 : (g + 1) * 128].astype(F32)
                    part = part + xf * xf
                sq = jnp.sum(part.T, axis=0, keepdims=True)
                squares[i] = sq
            else:
                sq = squares[i]
            member = av[p : p + 1, rows] == own
            picked = jnp.sum(jnp.where(member, energy, 0.0), axis=0, keepdims=True)
            nearest = jnp.min(energy, axis=0, keepdims=True)
            weights = 1.0 / (1.0 + (sq + picked) / D)
            wm = jnp.where(member, weights, 0.0)
            high = wm.astype(BF16)
            wv[0:NK, rows] = high
            wv[NK : 2 * NK, rows] = (wm - high.astype(F32)).astype(BF16)
            for g in range(CH // 128):
                cacc[...] += wm[:, g * 128 : (g + 1) * 128]
            for g in range(CH // GP):
                pn[i * (CH // GP) + g, 2 * p : 2 * p + 1, :] = picked[:, g * GP : (g + 1) * GP]
                pn[i * (CH // GP) + g, 2 * p + 1 : 2 * p + 2, :] = nearest[:, g * GP : (g + 1) * GP]

        def body(i, carry):
            multiply(i + 1)
            select(i)
            return carry

        multiply(0)
        lax.fori_loop(0, STEPS - 1, body, 0)
        select(STEPS - 1)

    def block(b):
        cols = pl.multiple_of(b * 128, 128)
        rhs = jnp.concatenate([xv[:, pl.ds(cols, 128)], xv[:, pl.ds(512 + cols, 128)]], axis=1)
        both = jnp.dot(wv[...], rhs, preferred_element_type=F32)
        return (both[:NK] + both[NK:]).T

    share = x * NY + y
    turned = jnp.concatenate([cv[:, 0:512], cv[:, 512:1024]], axis=0).T
    cpack[...] = turned
    of = lax.broadcasted_iota(jnp.int32, (128, NK), 0)
    pick_a = (of == kv[...]).astype(F32)
    pick_b = (of == kv[...] + NC).astype(F32)
    coarse = cpack[pl.ds(pl.multiple_of(share * 16, 16), 16), :]

    for p in range(PASSES):
        last = p == PASSES - 1
        with jax.named_scope(f'energies{p}'):
            energies(p)
        if last:
            pn_copies = [
                remote(pn.at[(cen + d) % NCEN], pn_recv.at[d], p_s.at[d], p_r.at[d], c_peer(d))
                for d in range(1, NCEN)
            ]
        counts8 = jnp.sum(cacc[...].T.reshape(16, 8, NK), axis=0)

        t = block(x_far)
        if p == 0:
            with jax.named_scope('w_barrier'):
                pl.semaphore_wait(barrier, 2 + (NY - 1) + (NCEN - 1))
        ahead[p, 0:8, :] = counts8
        ahead[p, 8:ROWS, :] = t
        h1 = remote(ahead.at[p, 0:FIRST], hop_r.at[p], rs_s.at[p, 0], rs_r.at[p, 0], right)
        h2 = remote(ahead.at[p, FIRST:ROWS], hop_l.at[p], rs_s.at[p, 1], rs_r.at[p, 1], left)
        t = block(x_right)
        blk_r[p, FIRST:ROWS, :] = t[128:]
        r2 = remote(
            blk_r.at[p, FIRST:ROWS], got_l.at[p, FIRST:ROWS], rs_s.at[p, 2], rs_r.at[p, 2], right
        )
        blk_r[p, 0:8, :] = counts8
        blk_r[p, 8:FIRST, :] = t[:128]
        t = block(x_left)
        blk_l[p, 0:8, :] = counts8
        blk_l[p, 8:FIRST, :] = t[:128]
        l1 = remote(blk_l.at[p, 0:FIRST], got_r.at[p, 0:FIRST], rs_s.at[p, 3], rs_r.at[p, 3], left)
        arrive('w_h1', h1)
        blk_r[p, 0:FIRST, :] += hop_r[p]
        r1 = remote(blk_r.at[p, 0:FIRST], got_l.at[p, 0:FIRST], rs_s.at[p, 4], rs_r.at[p, 4], right)
        arrive('w_h2', h2)
        blk_l[p, FIRST:ROWS, :] = t[128:] + hop_l[p]
        l2 = remote(
            blk_l.at[p, FIRST:ROWS], got_r.at[p, FIRST:ROWS], rs_s.at[p, 5], rs_r.at[p, 5], left
        )
        t = block(x)
        arrive('w_rsx', r2, l1, r1, l2)
        counts8 = counts8 + got_l[p, 0:8, :] + got_r[p, 0:8, :]
        t = t + got_l[p, 8:ROWS, :] + got_r[p, 8:ROWS, :]
        for k in range(NY):
            ysend[p, k, 0:16, :] = t[k * 16 : (k + 1) * 16]
            ysend[p, k, 16:32, :] = t[128 + k * 16 : 128 + (k + 1) * 16]
            ysend[p, k, 32:40, :] = counts8
        ycopies = [
            remote(ysend.at[p, (y + d) % NY], yrecv.at[p, d], ys_s.at[p, d], ys_r.at[p, d], y_peer(d))
            for d in range(1, NY)
        ]
        if p > 0:
            coarse = coarse_update(ccopies, crecv, p - 1, coarse)
        lookup = jnp.concatenate(
            [
                jnp.dot(coarse, pick_a, precision=HIGH, preferred_element_type=F32),
                jnp.dot(coarse, pick_b, precision=HIGH, preferred_element_type=F32),
            ],
            axis=0,
        )
        if last:
            finish = pn[cen]
            picked0, near0, picked1, near1 = (finish[k : k + 1] for k in range(4))
            arrive('w_pn', *pn_copies)
            for d in range(1, NCEN):
                picked0 = picked0 + pn_recv[d, 0:1, :]
                near0 = jnp.minimum(near0, pn_recv[d, 1:2, :])
                picked1 = picked1 + pn_recv[d, 2:3, :]
                near1 = jnp.minimum(near1, pn_recv[d, 3:4, :])
            gap_g[cen, 0:1, :] = (picked0 - near0) / 32.0
            gap_g[cen, 1:2, :] = (picked1 - near1) / 32.0
            gap_copies = [
                remote(gap_g.at[cen], gap_g.at[cen], g_s.at[d], g_r.at[d], c_peer(d)) for d in range(1, NCEN)
            ]
        all_sum = ysend[p, y]
        arrive('w_rsy', *ycopies)
        for d in range(1, NY):
            all_sum = all_sum + yrecv[p, d]
        counts = jnp.sum(all_sum[32:40], axis=0, keepdims=True)
        fine = (all_sum[0:32] + PRIOR * lookup) / (counts + PRIOR)
        fine_g[p, x, y] = fine
        gy = [
            remote(fine_g.at[p, x, y], fine_g.at[p, x, y], gy_s.at[p, d], gy_r.at[p, d], y_peer(d))
            for d in range(1, NY)
        ]
        weighted = counts * fine
        crecv[p, cen, 0:16, :] = dot_nt(weighted[0:16], pick_a) + dot_nt(weighted[16:32], pick_b)
        crecv[p, cen, 16:24, :] = dot_nt(jnp.broadcast_to(counts, (8, NK)), pick_a + pick_b)
        ccopies = [
            remote(crecv.at[p, cen], crecv.at[p, cen], cs_s.at[p, d], cs_r.at[p, d], c_peer(d))
            for d in range(1, NCEN)
        ]
        arrive('w_gy', *gy)
        lo, hi = pl.ds(0, NY // 2), pl.ds(NY // 2, NY // 2)

        def to(where, half, sem):
            ref = fine_g.at[p, x, half]
            return remote(ref, ref, gx_s.at[p, sem], gx_r.at[p, sem], where)

        r_lo = to(right, lo, 0)
        l_hi = to(left, hi, 1)
        r_hi = to(right, hi, 2)
        l_lo = to(left, lo, 3)
        if last:
            coarse = coarse_update(ccopies, crecv, p, coarse)
            coarse_g[x, y] = coarse
            cy = [
                remote(coarse_g.at[x, y], coarse_g.at[x, y], cy_s.at[d], cy_r.at[d], y_peer(d))
                for d in range(1, NY)
            ]
        arrive('w_rlo', r_lo)
        ref = fine_g.at[p, x_left, lo]
        f_r = remote(ref, ref, gx_s.at[p, 4], gx_r.at[p, 4], right)
        arrive('w_lhi', l_hi)
        ref = fine_g.at[p, x_right, hi]
        f_l = remote(ref, ref, gx_s.at[p, 5], gx_r.at[p, 5], left)
        if last:
            arrive('w_cy', *cy)

            def coarse_to(where, half, sem):
                ref = coarse_g.at[x, half]
                return remote(ref, ref, cx_s.at[sem], cx_r.at[sem], where)

            cr_lo = coarse_to(right, lo, 0)
            cl_hi = coarse_to(left, hi, 1)
            cr_hi = coarse_to(right, hi, 2)
            cl_lo = coarse_to(left, lo, 3)
            arrive('w_gap', *gap_copies)
            for c in range(NCEN):
                gaps_out[:, c * GP : (c + 1) * GP] = gap_g[c]
            g_write = pltpu.make_async_copy(gaps_out, gaps_hbm, out_sem.at[2])
            g_write.start()
        arrive('w_gx', r_hi, l_lo, f_r, f_l)
        if last:
            arrive('w_crlo', cr_lo)
            ref = coarse_g.at[x_left, lo]
            cf_r = remote(ref, ref, cx_s.at[4], cx_r.at[4], right)
            arrive('w_clhi', cl_hi)
            ref = coarse_g.at[x_right, hi]
            cf_l = remote(ref, ref, cx_s.at[5], cx_r.at[5], left)
        total = jnp.zeros((1, NK), F32)
        for b in range(D // 128):
            h, bx = divmod(b, NX)
            t = fine_g[p, bx, :, h * 16 : (h + 1) * 16, :].reshape(128, NK)
            if last:
                fine_out[:, b * 128 : (b + 1) * 128] = t.T
            else:
                low[b * 128 : (b + 1) * 128, :] = t.astype(BF16)
                total = total + jnp.sum(t * t, axis=0, keepdims=True)
        if last:
            f_write = pltpu.make_async_copy(fine_out, fine_hbm, out_sem.at[0])
            f_write.start()
        else:
            norm[...] = total

    arrive('w_cx', cr_hi, cl_lo, cf_r, cf_l)
    t = coarse_g[...].reshape(512, 128).T
    coarse_out[:, 0:512] = t[0:NC]
    coarse_out[:, 512:1024] = t[NC : 2 * NC]
    c_write = pltpu.make_async_copy(coarse_out, coarse_hbm, out_sem.at[1])
    c_write.start()
    with jax.named_scope('w_sends'):
        for copy in sends:
            copy.wait_send()
    for copy in (g_write, f_write, c_write):
        copy.wait()


def coarse_update(copies, crecv, p, coarse):
    with jax.named_scope('w_coarse'):
        for copy in copies:
            copy.wait_recv()
    total = crecv[p, 0]
    for c in range(1, NCEN):
        total = total + crecv[p, c]
    return (total[0:16] + PRIOR * coarse) / (total[16:17] + PRIOR)


def write_out(fine, coarse, gaps, fine_hbm, coarse_hbm, gaps_hbm, fine_v, coarse_v, gaps_v, sem):
    through = ((fine, fine_v, fine_hbm), (coarse, coarse_v, coarse_hbm), (gaps, gaps_v, gaps_hbm))
    reads = [pltpu.make_async_copy(src, via, sem.at[0, i]) for i, (src, via, _) in enumerate(through)]
    writes = [pltpu.make_async_copy(via, dst, sem.at[1, i]) for i, (_, via, dst) in enumerate(through)]
    for copy in reads:
        copy.start()
    for read, write in zip(reads, writes):
        read.wait()
        write.start()
    for copy in writes:
        copy.wait()


def on_device(points, fine_assign, fine_start, coarse_start, coarse_assign):
    dma = pltpu.SemaphoreType.DMA
    vmem = pltpu.VMEM
    n = PASSES
    scratch = [
        vmem((NP, D), BF16), vmem((PASSES, NP), jnp.int32), vmem((NK, D), F32), vmem((NC, D), F32),
        vmem((1, NK), jnp.int32), dma((STEPS + 4,)),
        vmem((D, NK), BF16), vmem((1, NK), F32), vmem((2, CH, NK), F32), vmem((STEPS, 1, CH), F32), vmem((2 * NK, NP), BF16),
        vmem((NK, 128), F32),
        vmem((n, ROWS, 128), F32), vmem((n, FIRST, 128), F32), vmem((n, 128, 128), F32),
        vmem((n, ROWS, 128), F32), vmem((n, ROWS, 128), F32), vmem((n, ROWS, 128), F32), vmem((n, ROWS, 128), F32),
        vmem((n, NY, 40, 128), F32), vmem((n, NY, 40, 128), F32),
        vmem((n, NX, NY, 32, 128), F32), vmem((512, 128), F32), vmem((n, NCEN, 24, 128), F32),
        vmem((NX, NY, 16, 128), F32),
        vmem((NCEN, 4, GP), F32), vmem((NCEN, 4, GP), F32), vmem((NCEN, 2, GP), F32),
        vmem((NK, D), F32), vmem((NC, D), F32), vmem((PASSES, NP), F32), dma((3,)),
        dma((n, 6)), dma((n, 6)), dma((n, NY)), dma((n, NY)), dma((n, NY)), dma((n, NY)),
        dma((n, 6)), dma((n, 6)), dma((n, NCEN)), dma((n, NCEN)), dma((NY,)), dma((NY,)),
        dma((6,)), dma((6,)), dma((NCEN,)), dma((NCEN,)), dma((NCEN,)), dma((NCEN,)),
    ]
    shapes = (
        jax.ShapeDtypeStruct((NK, D), F32),
        jax.ShapeDtypeStruct((NC, D), F32),
        jax.ShapeDtypeStruct((PASSES, NP), F32),
    )
    outs = pl.pallas_call(
        kernel,
        out_shape=shapes,
        in_specs=[pl.BlockSpec(memory_space=pl.ANY)] * 5,
        out_specs=[pl.BlockSpec(memory_space=pl.ANY)] * 3,
        scratch_shapes=scratch,
        compiler_params=pltpu.CompilerParams(
            collective_id=0, has_side_effects=True, vmem_limit_bytes=67043328
        ),
    )(points, fine_assign, fine_start, coarse_start, coarse_assign.reshape(1, NK))
    return tuple(pl.pallas_call(
        write_out,
        out_shape=shapes,
        in_specs=[pl.BlockSpec(memory_space=pl.ANY)] * 3,
        out_specs=[pl.BlockSpec(memory_space=pl.ANY)] * 3,
        scratch_shapes=[vmem((NK, D), F32), vmem((NC, D), F32), vmem((PASSES, NP), F32), dma((2, 3))],
        compiler_params=pltpu.CompilerParams(vmem_limit_bytes=67043328),
    )(*outs))


def solution(mesh):
    placed = (P("pts", None), P(None, "pts"), P("cen", None), P(), P("cen"))
    return jax.shard_map(
        on_device,
        mesh=mesh,
        in_specs=placed,
        out_specs=(P("cen", None), P(), P(None, "pts")),
        check_vma=False,
    )
```

```python
import jax
import jax.numpy as jnp
from jax import lax
from jax.experimental import pallas as pl
from jax.experimental.pallas import tpu as pltpu
from jax.sharding import PartitionSpec as P

NC = 64
PASSES = 2
PRIOR = 4.0
D = 1024
NP = 4096
NK = 128
NX, NY, NZ, NCEN = 4, 8, 8, 16
CH = 512
STEPS = NP // CH
GP = NP // NCEN
F32 = jnp.float32
BF16 = jnp.bfloat16
MESH = pl.DeviceIdType.MESH
HIGH = lax.Precision.HIGHEST


def dot_nt(a, b):
    return lax.dot_general(a, b, (((1,), (1,)), ((), ())), precision=HIGH, preferred_element_type=F32)


def kernel(
    points, assign, fine_start, coarse_start, coarse_assign,
    fine_hbm, coarse_hbm, gaps_hbm,
    xv, av, fv, cv, kv, in_sem,
    low, norm, prod_a, prod_b, squares, wv, cacc,
    far, hop_r, hop_l, blk_r, blk_l, got_l, got_r, own_s, ysend, yrecv,
    cnt_s, cnt_x, cnt_m, cnt_y,
    fine_g, cpack, crecv, zsum, cpart, coarse_g,
    pn, pn_recv, gap_g, fine_out, coarse_out, gaps_out, out_sem,
    rs_s, rs_r, ys_s, ys_r, gy_s, gy_r, gx_s, gx_r, cs_s, cs_r, cy_s, cy_r, cx_s, cx_r, p_s, p_r, g_s, g_r,
    nx_s, nx_r, ny_s, ny_r, cp_s, cp_r,
):
    pts = lax.axis_index("pts")
    cen = lax.axis_index("cen")
    y = pts // NX
    x = pts % NX
    z = cen // 2
    x_right, x_left, x_far = (x + 1) % NX, (x + 3) % NX, (x + 2) % NX
    right = {"pts": y * NX + x_right}
    left = {"pts": y * NX + x_left}
    beyond = {"pts": y * NX + x_far}
    partner = {"cen": cen + 1 - 2 * (cen % 2)}

    def y_peer(d):
        return {"pts": ((y + d) % NY) * NX + x}

    def c_peer(d):
        return {"cen": (cen + d) % NCEN}

    sends = []

    def arrive(name, *copies):
        with jax.named_scope(name):
            for copy in copies:
                copy.wait_recv()

    def remote(src, dst, s, r, where):
        copy = pltpu.make_async_remote_copy(
            src_ref=src, dst_ref=dst, send_sem=s, recv_sem=r, device_id=where, device_id_type=MESH
        )
        copy.start()
        sends.append(copy)
        return copy

    fine_in = pltpu.make_async_copy(fine_start, fv, in_sem.at[STEPS])
    fine_in.start()

    def x_copy(i):
        rows = pl.ds(pl.multiple_of(i * CH, CH), CH)
        return pltpu.make_async_copy(points.at[rows], xv.at[rows], in_sem.at[i])

    a_in = pltpu.make_async_copy(assign, av, in_sem.at[STEPS + 1])
    k_in = pltpu.make_async_copy(coarse_assign, kv, in_sem.at[STEPS + 2])
    c_in = pltpu.make_async_copy(coarse_start, cv, in_sem.at[STEPS + 3])
    a_in.start()
    k_in.start()
    c_in.start()
    for i in range(STEPS):
        x_copy(i).start()

    barrier = pltpu.get_barrier_semaphore()
    for where in [right, left, beyond] + [y_peer(d) for d in range(1, NY)] + [c_peer(d) for d in range(1, NCEN)]:
        pl.semaphore_signal(barrier, inc=1, device_id=where, device_id_type=MESH)

    with jax.named_scope('w_fine_in'):
        fine_in.wait()
    total = jnp.zeros((1, NK), F32)
    for b in range(D // 128):
        t = fv[:, b * 128 : (b + 1) * 128].T
        low[b * 128 : (b + 1) * 128, :] = t.astype(BF16)
        total = total + jnp.sum(t * t, axis=0, keepdims=True)
    norm[...] = total
    with jax.named_scope('w_ins'):
        a_in.wait()
        k_in.wait()
        c_in.wait()

    own = lax.broadcasted_iota(jnp.int32, (NK, CH), 0) + cen * NK

    def energies(p):
        cacc[...] = jnp.zeros_like(cacc)

        def multiply(i, prod):
            if p == 0:
                x_copy(i).wait()
            rows = pl.ds(pl.multiple_of(i * CH, CH), CH)
            prod[...] = jnp.dot(xv[rows, :], low[...], preferred_element_type=F32)

        def select(i, prod):
            rows = pl.ds(pl.multiple_of(i * CH, CH), CH)
            energy = (norm[...] - 2.0 * prod[...]).T
            if p == 0:
                part = jnp.zeros((CH, 128), F32)
                for g in range(D // 128):
                    xf = xv[rows, g * 128 : (g + 1) * 128].astype(F32)
                    part = part + xf * xf
                sq = jnp.sum(part.T, axis=0, keepdims=True)
                squares[i] = sq
            else:
                sq = squares[i]
            member = av[p : p + 1, rows] == own
            picked = jnp.sum(jnp.where(member, energy, 0.0), axis=0, keepdims=True)
            nearest = jnp.min(energy, axis=0, keepdims=True)
            weights = 1.0 / (1.0 + (sq + picked) / D)
            wm = jnp.where(member, weights, 0.0)
            high = wm.astype(BF16)
            wv[0:NK, rows] = high
            wv[NK : 2 * NK, rows] = (wm - high.astype(F32)).astype(BF16)
            for g in range(CH // 128):
                cacc[...] += wm[:, g * 128 : (g + 1) * 128]
            for g in range(CH // GP):
                pn[i * (CH // GP) + g, 2 * p : 2 * p + 1, :] = picked[:, g * GP : (g + 1) * GP]
                pn[i * (CH // GP) + g, 2 * p + 1 : 2 * p + 2, :] = nearest[:, g * GP : (g + 1) * GP]

        def body(i, carry):
            multiply(2 * i + 1, prod_b)
            select(2 * i, prod_a)
            multiply(2 * i + 2, prod_a)
            select(2 * i + 1, prod_b)
            return carry

        multiply(0, prod_a)
        lax.fori_loop(0, STEPS // 2 - 1, body, 0)
        multiply(STEPS - 1, prod_b)
        select(STEPS - 2, prod_a)
        select(STEPS - 1, prod_b)

    def pair(first, second, h):
        cols = [pl.ds(pl.multiple_of(h * 512 + b * 128, 128), 128) for b in (first, second)]
        rhs = jnp.concatenate([xv[:, cols[0]], xv[:, cols[1]]], axis=1)
        both = jnp.dot(wv[...], rhs, preferred_element_type=F32)
        return (both[:NK] + both[NK:]).T

    share = x * NY + y
    turned = jnp.concatenate([cv[:, 0:512], cv[:, 512:1024]], axis=0).T
    cpack[...] = turned
    of = lax.broadcasted_iota(jnp.int32, (128, NK), 0)
    pick_a = (of == kv[...]).astype(F32)
    pick_b = (of == kv[...] + NC).astype(F32)
    coarse = cpack[pl.ds(pl.multiple_of(share * 16, 16), 16), :]

    for p in range(PASSES):
        last = p == PASSES - 1
        with jax.named_scope(f'energies{p}'):
            energies(p)
        picks = (pick_a, pick_b)
        cnt = jnp.sum(cacc[...].T, axis=0, keepdims=True)
        cnt_s[p] = cnt
        LO, HI = pl.ds(0, 64), pl.ds(64, 64)

        hops = []
        for h in range(2):
            t = pair(x_far, x_right, h)
            far[p, h] = t[:128]
            blk_r[p, h] = t[128:]
            if p == 0 and h == 0:
                with jax.named_scope('w_barrier'):
                    pl.semaphore_wait(barrier, 3 + (NY - 1) + (NCEN - 1))
            to_r = remote(far.at[p, h, LO], hop_r.at[p, h], rs_s.at[p, h, 0], rs_r.at[p, h, 0], right)
            to_l = remote(far.at[p, h, HI], hop_l.at[p, h], rs_s.at[p, h, 1], rs_r.at[p, h, 1], left)
            r2 = remote(blk_r.at[p, h, HI], got_l.at[p, h, HI], rs_s.at[p, h, 2], rs_r.at[p, h, 2], right)
            if h == 0:
                ncopies = [
                    remote(cnt_s.at[p], cnt_x.at[p, k], nx_s.at[p, k], nx_r.at[p, k], where)
                    for k, where in enumerate((right, left, beyond))
                ]
            t = pair(x_left, x, h)
            blk_l[p, h] = t[:128]
            own_s[h] = t[128:]
            l1 = remote(blk_l.at[p, h, LO], got_r.at[p, h, LO], rs_s.at[p, h, 3], rs_r.at[p, h, 3], left)
            hops.append((to_r, to_l, r2, l1))
        if last:
            pn_copies = [
                remote(pn.at[(cen + d) % NCEN], pn_recv.at[d], p_s.at[d], p_r.at[d], c_peer(d))
                for d in range(1, NCEN)
            ]
        waits = []
        for h in range(2):
            to_r, to_l, r2, l1 = hops[h]
            arrive(f'w_hop{h}', to_r)
            blk_r[p, h, 0:64, :] += hop_r[p, h]
            r1 = remote(blk_r.at[p, h, LO], got_l.at[p, h, LO], rs_s.at[p, h, 4], rs_r.at[p, h, 4], right)
            arrive(f'w_hop{h}', to_l)
            blk_l[p, h, 64:128, :] += hop_l[p, h]
            l2 = remote(blk_l.at[p, h, HI], got_r.at[p, h, HI], rs_s.at[p, h, 5], rs_r.at[p, h, 5], left)
            waits.append((r2, l1, r1, l2))
        arrive('w_nx', *ncopies)
        cnt = cnt + cnt_x[p, 0] + cnt_x[p, 1] + cnt_x[p, 2]
        cnt_m[p] = cnt
        mcopies = [
            remote(cnt_m.at[p], cnt_y.at[p, d], ny_s.at[p, d], ny_r.at[p, d], y_peer(d)) for d in range(1, NY)
        ]
        ycopies = []
        for h in range(2):
            arrive(f'w_rsx{h}', *waits[h])
            ysend[p, h] = (own_s[h] + got_l[p, h] + got_r[p, h]).reshape(NY, 16, 128)
            ycopies.append([
                remote(
                    ysend.at[p, h, (y + d) % NY], yrecv.at[p, h, d], ys_s.at[p, h, d], ys_r.at[p, h, d], y_peer(d)
                )
                for d in range(1, NY)
            ])
        if p > 0:
            coarse = coarse_update([pcopy], zsum, cpart, p - 1, coarse)
        lookups = [jnp.dot(coarse, pick, precision=HIGH, preferred_element_type=F32) for pick in picks]
        if last:
            finish = pn[cen]
            picked0, near0, picked1, near1 = (finish[k : k + 1] for k in range(4))
            arrive('w_pn', *pn_copies)
            for d in range(1, NCEN):
                picked0 = picked0 + pn_recv[d, 0:1, :]
                near0 = jnp.minimum(near0, pn_recv[d, 1:2, :])
                picked1 = picked1 + pn_recv[d, 2:3, :]
                near1 = jnp.minimum(near1, pn_recv[d, 3:4, :])
            gap_g[cen, 0:1, :] = (picked0 - near0) / 32.0
            gap_g[cen, 1:2, :] = (picked1 - near1) / 32.0
            gap_copies = [
                remote(gap_g.at[cen], gap_g.at[cen], g_s.at[d], g_r.at[d], c_peer(d)) for d in range(1, NCEN)
            ]
        arrive('w_ny', *mcopies)
        counts = cnt
        for d in range(1, NY):
            counts = counts + cnt_y[p, d]
        part = None
        gy = []
        for h in range(2):
            arrive(f'w_rsy{h}', *ycopies[h])
            total = ysend[p, h, y]
            for d in range(1, NY):
                total = total + yrecv[p, h, d]
            fine = (total + PRIOR * lookups[h]) / (counts + PRIOR)
            fine_g[p, h, x, y] = fine
            ref = fine_g.at[p, h, x, y]
            gy.append([remote(ref, ref, gy_s.at[p, h, d], gy_r.at[p, h, d], y_peer(d)) for d in range(1, NY)])
            weighted = dot_nt(counts * fine, picks[h])
            part = weighted if part is None else part + weighted
        crecv[p, z, 0:16, :] = part
        crecv[p, z, 16:24, :] = dot_nt(jnp.broadcast_to(counts, (8, NK)), pick_a + pick_b)
        ccopies = [
            remote(crecv.at[p, z], crecv.at[p, z], cs_s.at[p, d], cs_r.at[p, d], c_peer(2 * d))
            for d in range(1, NZ)
        ]
        lo, hi = pl.ds(0, NY // 2), pl.ds(NY // 2, NY // 2)
        firsts = []
        for h in range(2):
            arrive(f'w_gy{h}', *gy[h])

            def to(where, half, sem, h=h):
                ref = fine_g.at[p, h, x, half]
                return remote(ref, ref, gx_s.at[p, h, sem], gx_r.at[p, h, sem], where)

            firsts.append((to(right, lo, 0), to(left, hi, 1), to(right, hi, 2), to(left, lo, 3)))
        ends = []

        def forward(h):
            r_lo, l_hi, r_hi, l_lo = firsts[h]
            arrive(f'w_gx{h}', r_lo)
            ref = fine_g.at[p, h, x_left, lo]
            f_r = remote(ref, ref, gx_s.at[p, h, 4], gx_r.at[p, h, 4], right)
            arrive(f'w_gx{h}', l_hi)
            ref = fine_g.at[p, h, x_right, hi]
            f_l = remote(ref, ref, gx_s.at[p, h, 5], gx_r.at[p, h, 5], left)
            ends.extend((r_hi, l_lo, f_r, f_l))

        def chip_sum():
            arrive('w_cz', *ccopies)
            total = crecv[p, 0]
            for c in range(1, NZ):
                total = total + crecv[p, c]
            zsum[p] = total
            return remote(zsum.at[p], cpart.at[p], cp_s.at[p], cp_r.at[p], partner)

        if not last:
            forward(0)
            forward(1)
            pcopy = chip_sum()
        else:
            forward(0)
            pcopy = chip_sum()
            forward(1)
            coarse = coarse_update([pcopy], zsum, cpart, p, coarse)
            coarse_g[x, y] = coarse
            cy = [
                remote(coarse_g.at[x, y], coarse_g.at[x, y], cy_s.at[d], cy_r.at[d], y_peer(d))
                for d in range(1, NY)
            ]
            arrive('w_gap', *gap_copies)
            for c in range(NCEN):
                gaps_out[:, c * GP : (c + 1) * GP] = gap_g[c]
            g_write = pltpu.make_async_copy(gaps_out, gaps_hbm, out_sem.at[2])
            g_write.start()
            arrive('w_cy', *cy)

            def coarse_to(where, half, sem):
                ref = coarse_g.at[x, half]
                return remote(ref, ref, cx_s.at[sem], cx_r.at[sem], where)

            cr_lo = coarse_to(right, lo, 0)
            cl_hi = coarse_to(left, hi, 1)
            cr_hi = coarse_to(right, hi, 2)
            cl_lo = coarse_to(left, lo, 3)
        arrive('w_gx', *ends)
        total = jnp.zeros((1, NK), F32)
        for b in range(D // 128):
            h, bx = divmod(b, NX)
            t = fine_g[p, h, bx].reshape(128, NK)
            if last:
                fine_out[:, b * 128 : (b + 1) * 128] = t.T
            else:
                low[b * 128 : (b + 1) * 128, :] = t.astype(BF16)
                total = total + jnp.sum(t * t, axis=0, keepdims=True)
        if last:
            f_write = pltpu.make_async_copy(fine_out, fine_hbm, out_sem.at[0])
            f_write.start()
            arrive('w_crlo', cr_lo)
            ref = coarse_g.at[x_left, lo]
            cf_r = remote(ref, ref, cx_s.at[4], cx_r.at[4], right)
            arrive('w_clhi', cl_hi)
            ref = coarse_g.at[x_right, hi]
            cf_l = remote(ref, ref, cx_s.at[5], cx_r.at[5], left)
        else:
            norm[...] = total

    arrive('w_cx', cr_hi, cl_lo, cf_r, cf_l)
    t = coarse_g[...].reshape(512, 128).T
    coarse_out[:, 0:512] = t[0:NC]
    coarse_out[:, 512:1024] = t[NC : 2 * NC]
    c_write = pltpu.make_async_copy(coarse_out, coarse_hbm, out_sem.at[1])
    c_write.start()
    with jax.named_scope('w_sends'):
        for copy in sends:
            copy.wait_send()
    for copy in (g_write, f_write, c_write):
        copy.wait()


def coarse_update(copies, zsum, cpart, p, coarse):
    with jax.named_scope('w_coarse'):
        for copy in copies:
            copy.wait_recv()
    total = zsum[p] + cpart[p]
    return (total[0:16] + PRIOR * coarse) / (total[16:17] + PRIOR)


def write_out(fine, coarse, gaps, fine_hbm, coarse_hbm, gaps_hbm, fine_v, coarse_v, gaps_v, sem):
    through = ((fine, fine_v, fine_hbm), (coarse, coarse_v, coarse_hbm), (gaps, gaps_v, gaps_hbm))
    reads = [pltpu.make_async_copy(src, via, sem.at[0, i]) for i, (src, via, _) in enumerate(through)]
    writes = [pltpu.make_async_copy(via, dst, sem.at[1, i]) for i, (_, via, dst) in enumerate(through)]
    for copy in reads:
        copy.start()
    for read, write in zip(reads, writes):
        read.wait()
        write.start()
    for copy in writes:
        copy.wait()


def on_device(points, fine_assign, fine_start, coarse_start, coarse_assign):
    dma = pltpu.SemaphoreType.DMA
    vmem = pltpu.VMEM
    n = PASSES
    scratch = [
        vmem((NP, D), BF16), vmem((PASSES, NP), jnp.int32), vmem((NK, D), F32), vmem((NC, D), F32),
        vmem((1, NK), jnp.int32), dma((STEPS + 4,)),
        vmem((D, NK), BF16), vmem((1, NK), F32), vmem((CH, NK), F32), vmem((CH, NK), F32),
        vmem((STEPS, 1, CH), F32), vmem((2 * NK, NP), BF16), vmem((NK, 128), F32),
        vmem((n, 2, 128, 128), F32), vmem((n, 2, 64, 128), F32), vmem((n, 2, 64, 128), F32),
        vmem((n, 2, 128, 128), F32), vmem((n, 2, 128, 128), F32), vmem((n, 2, 128, 128), F32),
        vmem((n, 2, 128, 128), F32), vmem((2, 128, 128), F32),
        vmem((n, 2, NY, 16, 128), F32), vmem((n, 2, NY, 16, 128), F32),
        vmem((n, 1, 128), F32), vmem((n, 3, 1, 128), F32), vmem((n, 1, 128), F32), vmem((n, NY, 1, 128), F32),
        vmem((n, 2, NX, NY, 16, 128), F32), vmem((512, 128), F32), vmem((n, NZ, 24, 128), F32),
        vmem((n, 24, 128), F32), vmem((n, 24, 128), F32), vmem((NX, NY, 16, 128), F32),
        vmem((NCEN, 4, GP), F32), vmem((NCEN, 4, GP), F32), vmem((NCEN, 2, GP), F32),
        vmem((NK, D), F32), vmem((NC, D), F32), vmem((PASSES, NP), F32), dma((3,)),
        dma((n, 2, 6)), dma((n, 2, 6)), dma((n, 2, NY)), dma((n, 2, NY)), dma((n, 2, NY)), dma((n, 2, NY)),
        dma((n, 2, 6)), dma((n, 2, 6)), dma((n, NZ)), dma((n, NZ)), dma((NY,)), dma((NY,)),
        dma((6,)), dma((6,)), dma((NCEN,)), dma((NCEN,)), dma((NCEN,)), dma((NCEN,)),
        dma((n, 3)), dma((n, 3)), dma((n, NY)), dma((n, NY)), dma((n,)), dma((n,)),
    ]
    shapes = (
        jax.ShapeDtypeStruct((NK, D), F32),
        jax.ShapeDtypeStruct((NC, D), F32),
        jax.ShapeDtypeStruct((PASSES, NP), F32),
    )
    outs = pl.pallas_call(
        kernel,
        out_shape=shapes,
        in_specs=[pl.BlockSpec(memory_space=pl.ANY)] * 5,
        out_specs=[pl.BlockSpec(memory_space=pl.ANY)] * 3,
        scratch_shapes=scratch,
        compiler_params=pltpu.CompilerParams(
            collective_id=0, has_side_effects=True, vmem_limit_bytes=67043328
        ),
    )(points, fine_assign, fine_start, coarse_start, coarse_assign.reshape(1, NK))
    return tuple(pl.pallas_call(
        write_out,
        out_shape=shapes,
        in_specs=[pl.BlockSpec(memory_space=pl.ANY)] * 3,
        out_specs=[pl.BlockSpec(memory_space=pl.ANY)] * 3,
        scratch_shapes=[vmem((NK, D), F32), vmem((NC, D), F32), vmem((PASSES, NP), F32), dma((2, 3))],
        compiler_params=pltpu.CompilerParams(vmem_limit_bytes=67043328),
    )(*outs))


def solution(mesh):
    placed = (P("pts", None), P(None, "pts"), P("cen", None), P(), P("cen"))
    return jax.shard_map(
        on_device,
        mesh=mesh,
        in_specs=placed,
        out_specs=(P("cen", None), P(), P(None, "pts")),
        check_vma=False,
    )
```

```python
import jax
import jax.numpy as jnp
from jax import lax
from jax.experimental import pallas as pl
from jax.experimental.pallas import tpu as pltpu
from jax.sharding import PartitionSpec as P

NC = 64
PASSES = 2
PRIOR = 4.0
D = 1024
NP = 4096
NK = 128
NX, NY, NCEN = 4, 8, 16
CH = 512
STEPS = NP // CH
GP = NP // NCEN
F32 = jnp.float32
BF16 = jnp.bfloat16
MESH = pl.DeviceIdType.MESH
HIGH = lax.Precision.HIGHEST


def dot_nt(a, b):
    return lax.dot_general(a, b, (((1,), (1,)), ((), ())), precision=HIGH, preferred_element_type=F32)


def kernel(
    points, assign, fine_start, coarse_start, coarse_assign,
    fine_hbm, coarse_hbm, gaps_hbm,
    xv, av, fv, cv, kv, in_sem,
    low, norm, prod_a, prod_b, squares, wv, cacc,
    far, hop_r, hop_l, blk_r, blk_l, got_l, got_r, own_s, ysend, yrecv,
    cnt_s, cnt_x, cnt_m, cnt_y,
    fine_g, cpack, crecv, ccnt, halves, coarse_g,
    pn, pn_recv, gap_g, fine_out, coarse_out, gaps_out, out_sem,
    rs_s, rs_r, ys_s, ys_r, gy_s, gy_r, gx_s, gx_r, cs_s, cs_r, cn_s, cn_r, nx_s, nx_r, ny_s, ny_r,
    cy_s, cy_r, cx_s, cx_r, p_s, p_r, g_s, g_r, cp_s, cp_r,
):
    pts = lax.axis_index("pts")
    cen = lax.axis_index("cen")
    y = pts // NX
    x = pts % NX
    core = cen % 2
    x_right, x_left, x_far = (x + 1) % NX, (x + 3) % NX, (x + 2) % NX
    right = {"pts": y * NX + x_right}
    left = {"pts": y * NX + x_left}
    beyond = {"pts": y * NX + x_far}
    partner = {"cen": cen + 1 - 2 * core}

    def y_peer(d):
        return {"pts": ((y + d) % NY) * NX + x}

    def c_peer(d):
        return {"cen": (cen + d) % NCEN}

    sent = []

    def remote(src, dst, s, r, where):
        copy = pltpu.make_async_remote_copy(
            src_ref=src, dst_ref=dst, send_sem=s, recv_sem=r, device_id=where, device_id_type=MESH
        )
        copy.start()

    def waiter(ref, sem):
        return pltpu.make_async_remote_copy(
            src_ref=ref, dst_ref=ref, send_sem=sem, recv_sem=sem, device_id=right, device_id_type=MESH
        )

    def arrive(name, ref, sem):
        with jax.named_scope(name):
            waiter(ref, sem).wait_recv()

    def to_send(ref, sem):
        sent.append(waiter(ref, sem))

    fine_in = pltpu.make_async_copy(fine_start, fv, in_sem.at[STEPS])
    fine_in.start()

    def x_copy(i):
        rows = pl.ds(pl.multiple_of(i * CH, CH), CH)
        return pltpu.make_async_copy(points.at[rows], xv.at[rows, pl.ds(0, D)], in_sem.at[i])

    a_in = pltpu.make_async_copy(assign, av, in_sem.at[STEPS + 1])
    k_in = pltpu.make_async_copy(coarse_assign, kv, in_sem.at[STEPS + 2])
    c_in = pltpu.make_async_copy(coarse_start, cv, in_sem.at[STEPS + 3])
    a_in.start()
    k_in.start()
    c_in.start()
    for i in range(STEPS):
        x_copy(i).start()

    barrier = pltpu.get_barrier_semaphore()
    for where in [right, left, beyond] + [y_peer(d) for d in range(1, NY)] + [c_peer(d) for d in range(1, NCEN)]:
        pl.semaphore_signal(barrier, inc=1, device_id=where, device_id_type=MESH)

    with jax.named_scope('w_fine_in'):
        fine_in.wait()
    total = jnp.zeros((1, NK), F32)
    for b in range(D // 128):
        t = fv[:, b * 128 : (b + 1) * 128].T
        low[b * 128 : (b + 1) * 128, :] = t.astype(BF16)
        total = total + jnp.sum(t * t, axis=0, keepdims=True)
    norm[...] = total
    with jax.named_scope('w_ins'):
        a_in.wait()
        k_in.wait()
        c_in.wait()

    own = lax.broadcasted_iota(jnp.int32, (NK, 128), 0) + cen * NK

    def energies(p):
        cacc[...] = jnp.zeros_like(cacc)

        def multiply(i, prod):
            if p == 0:
                x_copy(i).wait()
            rows = pl.ds(pl.multiple_of(i * CH, CH), CH)
            prod[...] = jnp.dot(xv[rows, 0:D], low[...], preferred_element_type=F32)

        def select(i, prod):
            for g in range(CH // 128):
                here = slice(g * 128, (g + 1) * 128)
                rows = pl.ds(pl.multiple_of(i * CH + g * 128, 128), 128)
                energy = (norm[...] - 2.0 * prod[here, :]).T
                if p == 0:
                    part = jnp.zeros((128, 128), F32)
                    for f in range(D // 128):
                        xf = xv[rows, f * 128 : (f + 1) * 128].astype(F32)
                        part = part + xf * xf
                    sq = jnp.sum(part.T, axis=0, keepdims=True)
                    squares[i, :, here] = sq
                else:
                    sq = squares[i, :, here]
                member = av[p : p + 1, rows] == own
                picked = jnp.sum(jnp.where(member, energy, 0.0), axis=0, keepdims=True)
                nearest = jnp.min(energy, axis=0, keepdims=True)
                weights = 1.0 / (1.0 + (sq + picked) / D)
                wm = jnp.where(member, weights, 0.0)
                high = wm.astype(BF16)
                wv[0:NK, rows] = high
                wv[NK : 2 * NK, rows] = (wm - high.astype(F32)).astype(BF16)
                cacc[...] += wm
                at = i * (CH // GP) + g * 128 // GP
                lane = slice(g * 128 % GP, g * 128 % GP + 128)
                pn[at, 2 * p : 2 * p + 1, lane] = picked
                pn[at, 2 * p + 1 : 2 * p + 2, lane] = nearest

        def body(i, carry):
            multiply(2 * i + 1, prod_b)
            select(2 * i, prod_a)
            multiply(2 * i + 2, prod_a)
            select(2 * i + 1, prod_b)
            return carry

        multiply(0, prod_a)
        lax.fori_loop(0, STEPS // 2 - 1, body, 0)
        multiply(STEPS - 1, prod_b)
        select(STEPS - 2, prod_a)
        select(STEPS - 1, prod_b)

    def pair(first, second, h):
        cols = [pl.ds(pl.multiple_of(h * 512 + b * 128, 128), 128) for b in (first, second)]
        rhs = jnp.concatenate([xv[:, cols[0]], xv[:, cols[1]]], axis=1)
        both = jnp.dot(wv[:, 0:NP], rhs, preferred_element_type=F32)
        return (both[:NK] + both[NK:]).T

    share = x * NY + y
    turned = jnp.concatenate([cv[:, 0:512], cv[:, 512:1024]], axis=0).T
    cpack[...] = turned
    of = lax.broadcasted_iota(jnp.int32, (128, NK), 0)
    pick_a = (of == kv[...]).astype(F32)
    pick_b = (of == kv[...] + NC).astype(F32)
    coarse = cpack[pl.ds(pl.multiple_of(share * 16, 16), 16), :]

    for p in range(PASSES):
        last = p == PASSES - 1
        with jax.named_scope(f'energies{p}'):
            energies(p)
        picks = (pick_a, pick_b)
        cnt = jnp.sum(cacc[...].T, axis=0, keepdims=True)
        cnt_s[p] = cnt
        LO, HI = pl.ds(0, 64), pl.ds(64, 64)

        for h in range(2):
            ss, rr = rs_s.at[p, h], rs_r.at[p, h, 2]
            t = pair(x_far, x_right, h)
            far[p, h] = t[:128]
            blk_r[p, h] = t[128:]
            if p == 0 and h == 0:
                with jax.named_scope('w_barrier'):
                    pl.semaphore_wait(barrier, 3 + (NY - 1) + (NCEN - 1))
            remote(far.at[p, h, LO], hop_r.at[p, h], ss, rs_r.at[p, h, 0], right)
            remote(far.at[p, h, HI], hop_l.at[p, h], ss, rs_r.at[p, h, 1], left)
            remote(blk_r.at[p, h, HI], got_l.at[p, h, HI], ss, rr, right)
            if h == 0:
                for k, where in enumerate((right, left, beyond)):
                    remote(cnt_s.at[p], cnt_x.at[p, k], nx_s.at[p], nx_r.at[p], where)
                to_send(cnt_x.at[p], nx_s.at[p])
            t = pair(x_left, x, h)
            blk_l[p, h] = t[:128]
            own_s[h] = t[128:]
            remote(blk_l.at[p, h, LO], got_r.at[p, h, LO], ss, rr, left)
        if last:
            for d in range(1, NCEN):
                remote(pn.at[(cen + d) % NCEN], pn_recv.at[d], p_s.at[0], p_r.at[0], c_peer(d))
            to_send(pn_recv.at[pl.ds(1, NCEN - 1)], p_s.at[0])
        for h in range(2):
            ss, rr = rs_s.at[p, h], rs_r.at[p, h, 2]
            arrive(f'w_hop{h}', hop_r.at[p, h], rs_r.at[p, h, 0])
            blk_r[p, h, 0:64, :] += hop_r[p, h]
            remote(blk_r.at[p, h, LO], got_l.at[p, h, LO], ss, rr, right)
            arrive(f'w_hop{h}', hop_l.at[p, h], rs_r.at[p, h, 1])
            blk_l[p, h, 64:128, :] += hop_l[p, h]
            remote(blk_l.at[p, h, HI], got_r.at[p, h, HI], ss, rr, left)
            to_send(fine_g.at[p, h, pl.ds(0, 3)], ss)
        arrive('w_nx', cnt_x.at[p], nx_r.at[p])
        cnt = cnt + cnt_x[p, 0] + cnt_x[p, 1] + cnt_x[p, 2]
        cnt_m[p] = cnt
        for d in range(1, NY):
            remote(cnt_m.at[p], cnt_y.at[p, d], ny_s.at[p], ny_r.at[p], y_peer(d))
        others = pl.ds(1, NY - 1)
        to_send(cnt_y.at[p, others], ny_s.at[p])
        for h in range(2):
            arrive(f'w_rsx{h}', fine_g.at[p, h, pl.ds(0, 2)], rs_r.at[p, h, 2])
            ysend[p, h] = (own_s[h] + got_l[p, h] + got_r[p, h]).reshape(NY, 16, 128)
            for d in range(1, NY):
                remote(
                    ysend.at[p, h, (y + d) % NY], yrecv.at[p, h, d], ys_s.at[p, h], ys_r.at[p, h], y_peer(d)
                )
            to_send(yrecv.at[p, h, others], ys_s.at[p, h])
        if p > 0:
            arrive('w_coarse', crecv.at[p - 1, pl.ds(1, NCEN - 1)], cs_r.at[p - 1])
            arrive('w_coarse', ccnt.at[p - 1, pl.ds(1, NCEN - 1)], cn_r.at[p - 1])
            coarse = coarse_update(crecv[p - 1], ccnt[p - 1], coarse)
        lookups = [jnp.dot(coarse, pick, precision=HIGH, preferred_element_type=F32) for pick in picks]
        arrive('w_ny', cnt_y.at[p, others], ny_r.at[p])
        counts = cnt
        for d in range(1, NY):
            counts = counts + cnt_y[p, d]
        ccnt[p, cen] = dot_nt(jnp.broadcast_to(counts, (8, NK)), pick_a + pick_b)[0:1]
        for d in range(1, NCEN):
            remote(ccnt.at[p, cen], ccnt.at[p, cen], cn_s.at[p], cn_r.at[p], c_peer(d))
        to_send(ccnt.at[p, pl.ds(1, NCEN - 1)], cn_s.at[p])
        part = None
        for h in range(2):
            arrive(f'w_rsy{h}', yrecv.at[p, h, others], ys_r.at[p, h])
            total = ysend[p, h, y]
            for d in range(1, NY):
                total = total + yrecv[p, h, d]
            fine = (total + PRIOR * lookups[h]) / (counts + PRIOR)
            fine_g[p, h, x, y] = fine
            ref = fine_g.at[p, h, x, y]
            for d in range(1, NY):
                remote(ref, ref, gy_s.at[p, h], gy_r.at[p, h], y_peer(d))
            to_send(yrecv.at[p, h, others], gy_s.at[p, h])
            weighted = dot_nt(counts * fine, picks[h])
            part = weighted if part is None else part + weighted
        if last:
            mine = pl.ds(pl.multiple_of(core * 8, 8), 8)
            halves[0] = part
            halves[1] = coarse
            crecv[p, cen, 0:8, :] = halves[0, mine, :]
            for d in range(1, NCEN):
                theirs = pl.ds(pl.multiple_of((cen + d) % 2 * 8, 8), 8)
                remote(
                    halves.at[0, theirs], crecv.at[p, cen, pl.ds(0, 8)], cs_s.at[p], cs_r.at[p], c_peer(d)
                )
            some = crecv.at[p, pl.ds(1, NCEN - 1), pl.ds(0, 8)]
        else:
            crecv[p, cen] = part
            for d in range(1, NCEN):
                remote(crecv.at[p, cen], crecv.at[p, cen], cs_s.at[p], cs_r.at[p], c_peer(d))
            some = crecv.at[p, pl.ds(1, NCEN - 1)]
        to_send(some, cs_s.at[p])
        lo, hi = pl.ds(0, NY // 2), pl.ds(NY // 2, NY // 2)
        for h in range(2):
            arrive(f'w_gy{h}', yrecv.at[p, h, others], gy_r.at[p, h])
            low_half, high_half = fine_g.at[p, h, x, lo], fine_g.at[p, h, x, hi]
            ss = gx_s.at[p, h]
            remote(low_half, low_half, ss, gx_r.at[p, h, 0], right)
            remote(high_half, high_half, ss, gx_r.at[p, h, 1], left)
            remote(high_half, high_half, ss, gx_r.at[p, h, 2], right)
            remote(low_half, low_half, ss, gx_r.at[p, h, 2], left)

        def forward(h):
            ss, rr = gx_s.at[p, h], gx_r.at[p, h, 2]
            ref = fine_g.at[p, h, x_left, lo]
            arrive(f'w_gx{h}', ref, gx_r.at[p, h, 0])
            remote(ref, ref, ss, rr, right)
            ref = fine_g.at[p, h, x_right, hi]
            arrive(f'w_gx{h}', ref, gx_r.at[p, h, 1])
            remote(ref, ref, ss, rr, left)
            to_send(fine_g.at[p, h, pl.ds(0, 3)], ss)

        forward(0)
        if last:
            arrive('w_coarse', some, cs_r.at[p])
            arrive('w_coarse', ccnt.at[p, pl.ds(1, NCEN - 1)], cn_r.at[p])
            coarse_g[core, x, y] = coarse_update(crecv[p, :, 0:8, :], ccnt[p], halves[1, mine, :])
            ref = coarse_g.at[core, x, y]
            for d in range(1, NY):
                remote(ref, ref, cy_s.at[0], cy_r.at[0], y_peer(d))
            to_send(coarse_g.at[0, 0, others], cy_s.at[0])
        forward(1)
        if last:
            finish = pn[cen]
            picked0, near0, picked1, near1 = (finish[k : k + 1] for k in range(4))
            arrive('w_pn', pn_recv.at[pl.ds(1, NCEN - 1)], p_r.at[0])
            for d in range(1, NCEN):
                picked0 = picked0 + pn_recv[d, 0:1, :]
                near0 = jnp.minimum(near0, pn_recv[d, 1:2, :])
                picked1 = picked1 + pn_recv[d, 2:3, :]
                near1 = jnp.minimum(near1, pn_recv[d, 3:4, :])
            gap_g[cen, 0:1, :] = (picked0 - near0) / 32.0
            gap_g[cen, 1:2, :] = (picked1 - near1) / 32.0
            for d in range(1, NCEN):
                remote(gap_g.at[cen], gap_g.at[cen], g_s.at[0], g_r.at[0], c_peer(d))
            to_send(gap_g.at[pl.ds(1, NCEN - 1)], g_s.at[0])
            arrive('w_cy', coarse_g.at[0, 0, others], cy_r.at[0])
            ref = coarse_g.at[core, x]
            for where in (right, left, beyond):
                remote(ref, ref, cx_s.at[0], cx_r.at[0], where)
            to_send(coarse_g.at[0, pl.ds(0, 3)], cx_s.at[0])
        total = jnp.zeros((1, NK), F32)
        for h in range(2):
            arrive('w_gx', fine_g.at[p, h, pl.ds(0, 2)], gx_r.at[p, h, 2])
            for bx in range(NX):
                b = h * NX + bx
                t = fine_g[p, h, bx].reshape(128, NK)
                if last:
                    fine_out[:, b * 128 : (b + 1) * 128] = t.T
                else:
                    low[b * 128 : (b + 1) * 128, :] = t.astype(BF16)
                    total = total + jnp.sum(t * t, axis=0, keepdims=True)
        if not last:
            norm[...] = total

    f_write = pltpu.make_async_copy(fine_out, fine_hbm, out_sem.at[0])
    f_write.start()
    arrive('w_cx', coarse_g.at[0, pl.ds(0, 3)], cx_r.at[0])
    ref = coarse_g.at[core]
    remote(ref, ref, cp_s.at[0], cp_r.at[0], partner)
    to_send(ref, cp_s.at[0])
    arrive('w_gap', gap_g.at[pl.ds(1, NCEN - 1)], g_r.at[0])
    for c in range(NCEN):
        gaps_out[:, c * GP : (c + 1) * GP] = gap_g[c]
    g_write = pltpu.make_async_copy(gaps_out, gaps_hbm, out_sem.at[2])
    g_write.start()
    arrive('w_cp', ref, cp_r.at[0])
    t = jnp.concatenate([coarse_g[c].reshape(NX * NY, 8, 128) for c in range(2)], axis=1).reshape(512, 128).T
    coarse_out[:, 0:512] = t[0:NC]
    coarse_out[:, 512:1024] = t[NC : 2 * NC]
    c_write = pltpu.make_async_copy(coarse_out, coarse_hbm, out_sem.at[1])
    c_write.start()
    with jax.named_scope('w_sends'):
        for copy in sent:
            copy.wait_send()
    for copy in (g_write, f_write, c_write):
        copy.wait()


def coarse_update(parts, counts, coarse):
    total, count = parts[0], counts[0]
    for c in range(1, NCEN):
        total = total + parts[c]
        count = count + counts[c]
    return (total + PRIOR * coarse) / (count + PRIOR)


def write_out(fine, coarse, gaps, fine_hbm, coarse_hbm, gaps_hbm, fine_v, coarse_v, gaps_v, sem):
    through = ((fine, fine_v, fine_hbm), (coarse, coarse_v, coarse_hbm), (gaps, gaps_v, gaps_hbm))
    reads = [pltpu.make_async_copy(src, via, sem.at[0, i]) for i, (src, via, _) in enumerate(through)]
    writes = [pltpu.make_async_copy(via, dst, sem.at[1, i]) for i, (_, via, dst) in enumerate(through)]
    for copy in reads:
        copy.start()
    for read, write in zip(reads, writes):
        read.wait()
        write.start()
    for copy in writes:
        copy.wait()


def on_device(points, fine_assign, fine_start, coarse_start, coarse_assign):
    dma = pltpu.SemaphoreType.DMA
    vmem = pltpu.VMEM
    n = PASSES
    scratch = [
        vmem((NP, D + 128), BF16), vmem((PASSES, NP), jnp.int32), vmem((NK, D), F32), vmem((NC, D), F32),
        vmem((1, NK), jnp.int32), dma((STEPS + 4,)),
        vmem((D, NK), BF16), vmem((1, NK), F32), vmem((CH, NK), F32), vmem((CH, NK), F32),
        vmem((STEPS, 1, CH), F32), vmem((2 * NK, NP + 128), BF16), vmem((NK, 128), F32),
        vmem((n, 2, 128, 128), F32), vmem((n, 2, 64, 128), F32), vmem((n, 2, 64, 128), F32),
        vmem((n, 2, 128, 128), F32), vmem((n, 2, 128, 128), F32), vmem((n, 2, 128, 128), F32),
        vmem((n, 2, 128, 128), F32), vmem((2, 128, 128), F32),
        vmem((n, 2, NY, 16, 128), F32), vmem((n, 2, NY, 16, 128), F32),
        vmem((n, 1, 128), F32), vmem((n, 3, 1, 128), F32), vmem((n, 1, 128), F32), vmem((n, NY, 1, 128), F32),
        vmem((n, 2, NX, NY, 16, 128), F32), vmem((512, 128), F32), vmem((n, NCEN, 16, 128), F32),
        vmem((n, NCEN, 1, 128), F32), vmem((2, 16, 128), F32), vmem((2, NX, NY, 8, 128), F32),
        vmem((NCEN, 4, GP), F32), vmem((NCEN, 4, GP), F32), vmem((NCEN, 2, GP), F32),
        vmem((NK, D), F32), vmem((NC, D), F32), vmem((PASSES, NP), F32), dma((3,)),
        dma((n, 2)), dma((n, 2, 3)), dma((n, 2)), dma((n, 2)), dma((n, 2)), dma((n, 2)), dma((n, 2)), dma((n, 2, 3)),
        *[dma((n,))] * 8, *[dma((1,))] * 10,
    ]
    shapes = (
        jax.ShapeDtypeStruct((NK, D), F32),
        jax.ShapeDtypeStruct((NC, D), F32),
        jax.ShapeDtypeStruct((PASSES, NP), F32),
    )
    outs = pl.pallas_call(
        kernel,
        out_shape=shapes,
        in_specs=[pl.BlockSpec(memory_space=pl.ANY)] * 5,
        out_specs=[pl.BlockSpec(memory_space=pl.ANY)] * 3,
        scratch_shapes=scratch,
        compiler_params=pltpu.CompilerParams(
            collective_id=0, has_side_effects=True, vmem_limit_bytes=67043328
        ),
    )(points, fine_assign, fine_start, coarse_start, coarse_assign.reshape(1, NK))
    return tuple(pl.pallas_call(
        write_out,
        out_shape=shapes,
        in_specs=[pl.BlockSpec(memory_space=pl.ANY)] * 3,
        out_specs=[pl.BlockSpec(memory_space=pl.ANY)] * 3,
        scratch_shapes=[vmem((NK, D), F32), vmem((NC, D), F32), vmem((PASSES, NP), F32), dma((2, 3))],
        compiler_params=pltpu.CompilerParams(vmem_limit_bytes=67043328),
    )(*outs))


def solution(mesh):
    placed = (P("pts", None), P(None, "pts"), P("cen", None), P(), P("cen"))
    return jax.shard_map(
        on_device,
        mesh=mesh,
        in_specs=placed,
        out_specs=(P("cen", None), P(), P(None, "pts")),
        check_vma=False,
    )
```

```python
import jax
import jax.numpy as jnp
from jax import lax
from jax.experimental import pallas as pl
from jax.experimental.pallas import tpu as pltpu
from jax.sharding import PartitionSpec as P

NC = 64
PASSES = 2
PRIOR = 4.0
D = 1024
NP = 4096
NK = 128
NX, NY, NCEN = 4, 8, 16
CH = 512
STEPS = NP // CH
GP = NP // NCEN
F32 = jnp.float32
BF16 = jnp.bfloat16
MESH = pl.DeviceIdType.MESH
HIGH = lax.Precision.HIGHEST


def dot_nt(a, b):
    return lax.dot_general(a, b, (((1,), (1,)), ((), ())), precision=HIGH, preferred_element_type=F32)


def kernel(
    points, assign, fine_start, coarse_start, coarse_assign,
    fine_hbm, coarse_hbm, gaps_hbm,
    xv, av, fv, cv, kv, in_sem,
    low, norm, prod_a, prod_b, squares, wv, cacc,
    far, hop_r, hop_l, blk_r, blk_l, got_l, got_r, own_s, ysend, yrecv,
    cnt_s, cnt_x, cnt_m, cnt_y,
    fine_g, cpack, crecv, ccnt, halves, coarse_g,
    pn, pn_recv, gap_g, fine_out, coarse_out, gaps_out, out_sem,
    rs_s, rs_r, ys_s, ys_r, gy_s, gy_r, gx_s, gx_r, cs_s, cs_r, cn_s, cn_r, nx_s, nx_r, ny_s, ny_r,
    cy_s, cy_r, cx_s, cx_r, p_s, p_r, g_s, g_r, cp_s, cp_r,
):
    pts = lax.axis_index("pts")
    cen = lax.axis_index("cen")
    y = pts // NX
    x = pts % NX
    core = cen % 2
    x_right, x_left, x_far = (x + 1) % NX, (x + 3) % NX, (x + 2) % NX
    right = {"pts": y * NX + x_right}
    left = {"pts": y * NX + x_left}
    beyond = {"pts": y * NX + x_far}
    partner = {"cen": cen + 1 - 2 * core}

    def y_peer(d):
        return {"pts": ((y + d) % NY) * NX + x}

    def c_peer(d):
        return {"cen": (cen + d) % NCEN}

    sent = []

    def remote(src, dst, s, r, where):
        copy = pltpu.make_async_remote_copy(
            src_ref=src, dst_ref=dst, send_sem=s, recv_sem=r, device_id=where, device_id_type=MESH
        )
        copy.start()

    def waiter(ref, sem):
        return pltpu.make_async_remote_copy(
            src_ref=ref, dst_ref=ref, send_sem=sem, recv_sem=sem, device_id=right, device_id_type=MESH
        )

    def arrive(name, ref, sem):
        with jax.named_scope(name):
            waiter(ref, sem).wait_recv()

    def to_send(ref, sem):
        sent.append(waiter(ref, sem))

    fine_in = pltpu.make_async_copy(fine_start, fv, in_sem.at[STEPS])
    fine_in.start()

    def x_copy(i):
        rows = pl.ds(pl.multiple_of(i * CH, CH), CH)
        return pltpu.make_async_copy(points.at[rows], xv.at[rows, pl.ds(0, D)], in_sem.at[i])

    a_in = pltpu.make_async_copy(assign, av, in_sem.at[STEPS + 1])
    k_in = pltpu.make_async_copy(coarse_assign, kv, in_sem.at[STEPS + 2])
    c_in = pltpu.make_async_copy(coarse_start, cv, in_sem.at[STEPS + 3])
    a_in.start()
    k_in.start()
    c_in.start()
    for i in range(STEPS):
        x_copy(i).start()

    barrier = pltpu.get_barrier_semaphore()
    for where in [right, left, beyond] + [y_peer(d) for d in range(1, NY)] + [c_peer(d) for d in range(1, NCEN)]:
        pl.semaphore_signal(barrier, inc=1, device_id=where, device_id_type=MESH)

    with jax.named_scope('w_fine_in'):
        fine_in.wait()
    total = jnp.zeros((1, NK), F32)
    for b in range(D // 128):
        t = fv[:, b * 128 : (b + 1) * 128].T
        low[b * 128 : (b + 1) * 128, :] = t.astype(BF16)
        total = total + jnp.sum(t * t, axis=0, keepdims=True)
    norm[...] = total
    with jax.named_scope('w_ins'):
        a_in.wait()
        k_in.wait()
        c_in.wait()

    own = lax.broadcasted_iota(jnp.int32, (NK, 128), 0) + cen * NK

    def energies(p):
        cacc[...] = jnp.zeros_like(cacc)

        def multiply(i, prod):
            if p == 0:
                x_copy(i).wait()
            rows = pl.ds(pl.multiple_of(i * CH, CH), CH)
            prod[...] = jnp.dot(xv[rows, 0:D], low[...], preferred_element_type=F32)

        def select(i, prod):
            for g in range(CH // 128):
                here = slice(g * 128, (g + 1) * 128)
                rows = pl.ds(pl.multiple_of(i * CH + g * 128, 128), 128)
                energy = (norm[...] - 2.0 * prod[here, :]).T
                if p == 0:
                    part = jnp.zeros((128, 128), F32)
                    for f in range(D // 128):
                        xf = xv[rows, f * 128 : (f + 1) * 128].astype(F32)
                        part = part + xf * xf
                    sq = jnp.sum(part.T, axis=0, keepdims=True)
                    squares[i, :, here] = sq
                else:
                    sq = squares[i, :, here]
                member = av[p : p + 1, rows] == own
                picked = jnp.sum(jnp.where(member, energy, 0.0), axis=0, keepdims=True)
                nearest = jnp.min(energy, axis=0, keepdims=True)
                weights = 1.0 / (1.0 + (sq + picked) / D)
                wm = jnp.where(member, weights, 0.0)
                high = wm.astype(BF16)
                wv[0:NK, rows] = high
                wv[NK : 2 * NK, rows] = (wm - high.astype(F32)).astype(BF16)
                cacc[...] += wm
                at = i * (CH // GP) + g * 128 // GP
                lane = slice(g * 128 % GP, g * 128 % GP + 128)
                pn[at, 2 * p : 2 * p + 1, lane] = picked
                pn[at, 2 * p + 1 : 2 * p + 2, lane] = nearest

        def body(i, carry):
            multiply(2 * i + 1, prod_b)
            select(2 * i, prod_a)
            multiply(2 * i + 2, prod_a)
            select(2 * i + 1, prod_b)
            return carry

        multiply(0, prod_a)
        lax.fori_loop(0, STEPS // 2 - 1, body, 0)
        multiply(STEPS - 1, prod_b)
        select(STEPS - 2, prod_a)
        select(STEPS - 1, prod_b)

    def pair(*which):
        cols = [pl.ds(pl.multiple_of(h * 512 + b * 128, 128), 128) for b, h in which]
        rhs = jnp.concatenate([xv[:, cols[0]], xv[:, cols[1]]], axis=1)
        both = jnp.dot(wv[:, 0:NP], rhs, preferred_element_type=F32)
        return (both[:NK] + both[NK:]).T

    share = x * NY + y
    turned = jnp.concatenate([cv[:, 0:512], cv[:, 512:1024]], axis=0).T
    cpack[...] = turned
    of = lax.broadcasted_iota(jnp.int32, (128, NK), 0)
    pick_a = (of == kv[...]).astype(F32)
    pick_b = (of == kv[...] + NC).astype(F32)
    coarse = cpack[pl.ds(pl.multiple_of(share * 16, 16), 16), :]

    for p in range(PASSES):
        last = p == PASSES - 1
        with jax.named_scope(f'energies{p}'):
            energies(p)
        picks = (pick_a, pick_b)
        cnt = jnp.sum(cacc[...].T, axis=0, keepdims=True)
        cnt_s[p] = cnt
        LO, HI = pl.ds(0, 64), pl.ds(64, 64)

        t = pair((x_far, 0), (x_far, 1))
        far[p, 0] = t[:128]
        far[p, 1] = t[128:]
        if p == 0:
            with jax.named_scope('w_barrier'):
                pl.semaphore_wait(barrier, 3 + (NY - 1) + (NCEN - 1))
        for h in range(2):
            remote(far.at[p, h, LO], hop_r.at[p, h], rs_s.at[p, h], rs_r.at[p, h, 0], right)
            remote(far.at[p, h, HI], hop_l.at[p, h], rs_s.at[p, h], rs_r.at[p, h, 1], left)
        for k, where in enumerate((right, left, beyond)):
            remote(cnt_s.at[p], cnt_x.at[p, k], nx_s.at[p], nx_r.at[p], where)
        to_send(cnt_x.at[p], nx_s.at[p])
        for h in range(2):
            t = pair((x_right, h), (x_left, h))
            blk_r[p, h] = t[:128]
            blk_l[p, h] = t[128:]
            ss, rr = rs_s.at[p, h], rs_r.at[p, h, 2]
            remote(blk_r.at[p, h, HI], got_l.at[p, h, HI], ss, rr, right)
            remote(blk_l.at[p, h, LO], got_r.at[p, h, LO], ss, rr, left)
        for h in range(2):
            ss, rr = rs_s.at[p, h], rs_r.at[p, h, 2]
            arrive(f'w_hop{h}', hop_r.at[p, h], rs_r.at[p, h, 0])
            blk_r[p, h, 0:64, :] += hop_r[p, h]
            remote(blk_r.at[p, h, LO], got_l.at[p, h, LO], ss, rr, right)
            arrive(f'w_hop{h}', hop_l.at[p, h], rs_r.at[p, h, 1])
            blk_l[p, h, 64:128, :] += hop_l[p, h]
            remote(blk_l.at[p, h, HI], got_r.at[p, h, HI], ss, rr, left)
            to_send(fine_g.at[p, h, pl.ds(0, 3)], ss)
        arrive('w_nx', cnt_x.at[p], nx_r.at[p])
        cnt = cnt + cnt_x[p, 0] + cnt_x[p, 1] + cnt_x[p, 2]
        cnt_m[p] = cnt
        for d in range(1, NY):
            remote(cnt_m.at[p], cnt_y.at[p, d], ny_s.at[p], ny_r.at[p], y_peer(d))
        others = pl.ds(1, NY - 1)
        to_send(cnt_y.at[p, others], ny_s.at[p])
        if last:
            for d in range(1, NCEN):
                remote(pn.at[(cen + d) % NCEN], pn_recv.at[d], p_s.at[0], p_r.at[0], c_peer(d))
            to_send(pn_recv.at[pl.ds(1, NCEN - 1)], p_s.at[0])
        t = pair((x, 0), (x, 1))
        own_s[0] = t[:128]
        own_s[1] = t[128:]
        for h in range(2):
            arrive(f'w_rsx{h}', fine_g.at[p, h, pl.ds(0, 2)], rs_r.at[p, h, 2])
            ysend[p, h] = (own_s[h] + got_l[p, h] + got_r[p, h]).reshape(NY, 16, 128)
            for d in range(1, NY):
                remote(
                    ysend.at[p, h, (y + d) % NY], yrecv.at[p, h, d], ys_s.at[p, h], ys_r.at[p, h], y_peer(d)
                )
            to_send(yrecv.at[p, h, others], ys_s.at[p, h])
        if p > 0:
            arrive('w_coarse', crecv.at[p - 1, pl.ds(1, NCEN - 1)], cs_r.at[p - 1])
            arrive('w_coarse', ccnt.at[p - 1, pl.ds(1, NCEN - 1)], cn_r.at[p - 1])
            coarse = coarse_update(crecv[p - 1], ccnt[p - 1], coarse)
        lookups = [jnp.dot(coarse, pick, precision=HIGH, preferred_element_type=F32) for pick in picks]
        arrive('w_ny', cnt_y.at[p, others], ny_r.at[p])
        counts = cnt
        for d in range(1, NY):
            counts = counts + cnt_y[p, d]
        ccnt[p, cen] = dot_nt(jnp.broadcast_to(counts, (8, NK)), pick_a + pick_b)[0:1]
        for d in range(1, NCEN):
            remote(ccnt.at[p, cen], ccnt.at[p, cen], cn_s.at[p], cn_r.at[p], c_peer(d))
        to_send(ccnt.at[p, pl.ds(1, NCEN - 1)], cn_s.at[p])
        part = None
        for h in range(2):
            arrive(f'w_rsy{h}', yrecv.at[p, h, others], ys_r.at[p, h])
            total = ysend[p, h, y]
            for d in range(1, NY):
                total = total + yrecv[p, h, d]
            fine = (total + PRIOR * lookups[h]) / (counts + PRIOR)
            fine_g[p, h, x, y] = fine
            ref = fine_g.at[p, h, x, y]
            for d in range(1, NY):
                remote(ref, ref, gy_s.at[p, h], gy_r.at[p, h], y_peer(d))
            to_send(yrecv.at[p, h, others], gy_s.at[p, h])
            weighted = dot_nt(counts * fine, picks[h])
            part = weighted if part is None else part + weighted
        if last:
            mine = pl.ds(pl.multiple_of(core * 8, 8), 8)
            halves[0] = part
            halves[1] = coarse
            crecv[p, cen, 0:8, :] = halves[0, mine, :]
            for d in range(1, NCEN):
                theirs = pl.ds(pl.multiple_of((cen + d) % 2 * 8, 8), 8)
                remote(
                    halves.at[0, theirs], crecv.at[p, cen, pl.ds(0, 8)], cs_s.at[p], cs_r.at[p], c_peer(d)
                )
            some = crecv.at[p, pl.ds(1, NCEN - 1), pl.ds(0, 8)]
        else:
            crecv[p, cen] = part
            for d in range(1, NCEN):
                remote(crecv.at[p, cen], crecv.at[p, cen], cs_s.at[p], cs_r.at[p], c_peer(d))
            some = crecv.at[p, pl.ds(1, NCEN - 1)]
        to_send(some, cs_s.at[p])
        lo, hi = pl.ds(0, NY // 2), pl.ds(NY // 2, NY // 2)
        for h in range(2):
            arrive(f'w_gy{h}', yrecv.at[p, h, others], gy_r.at[p, h])
            low_half, high_half = fine_g.at[p, h, x, lo], fine_g.at[p, h, x, hi]
            ss = gx_s.at[p, h]
            remote(low_half, low_half, ss, gx_r.at[p, h, 0], right)
            remote(high_half, high_half, ss, gx_r.at[p, h, 1], left)
            remote(high_half, high_half, ss, gx_r.at[p, h, 2], right)
            remote(low_half, low_half, ss, gx_r.at[p, h, 2], left)

        def forward(h):
            ss, rr = gx_s.at[p, h], gx_r.at[p, h, 2]
            ref = fine_g.at[p, h, x_left, lo]
            arrive(f'w_gx{h}', ref, gx_r.at[p, h, 0])
            remote(ref, ref, ss, rr, right)
            ref = fine_g.at[p, h, x_right, hi]
            arrive(f'w_gx{h}', ref, gx_r.at[p, h, 1])
            remote(ref, ref, ss, rr, left)
            to_send(fine_g.at[p, h, pl.ds(0, 3)], ss)

        forward(0)
        if last:
            arrive('w_coarse', some, cs_r.at[p])
            arrive('w_coarse', ccnt.at[p, pl.ds(1, NCEN - 1)], cn_r.at[p])
            coarse_g[core, x, y] = coarse_update(crecv[p, :, 0:8, :], ccnt[p], halves[1, mine, :])
            ref = coarse_g.at[core, x, y]
            for d in range(1, NY):
                remote(ref, ref, cy_s.at[0], cy_r.at[0], y_peer(d))
            to_send(coarse_g.at[0, 0, others], cy_s.at[0])
        forward(1)
        if last:
            finish = pn[cen]
            picked0, near0, picked1, near1 = (finish[k : k + 1] for k in range(4))
            arrive('w_pn', pn_recv.at[pl.ds(1, NCEN - 1)], p_r.at[0])
            for d in range(1, NCEN):
                picked0 = picked0 + pn_recv[d, 0:1, :]
                near0 = jnp.minimum(near0, pn_recv[d, 1:2, :])
                picked1 = picked1 + pn_recv[d, 2:3, :]
                near1 = jnp.minimum(near1, pn_recv[d, 3:4, :])
            gap_g[cen, 0:1, :] = (picked0 - near0) / 32.0
            gap_g[cen, 1:2, :] = (picked1 - near1) / 32.0
            for d in range(1, NCEN):
                remote(gap_g.at[cen], gap_g.at[cen], g_s.at[0], g_r.at[0], c_peer(d))
            to_send(gap_g.at[pl.ds(1, NCEN - 1)], g_s.at[0])
            arrive('w_cy', coarse_g.at[0, 0, others], cy_r.at[0])
            ref = coarse_g.at[core, x]
            for where in (right, left, beyond):
                remote(ref, ref, cx_s.at[0], cx_r.at[0], where)
            to_send(coarse_g.at[0, pl.ds(0, 3)], cx_s.at[0])
        total = jnp.zeros((1, NK), F32)
        for h in range(2):
            arrive('w_gx', fine_g.at[p, h, pl.ds(0, 2)], gx_r.at[p, h, 2])
            for bx in range(NX):
                b = h * NX + bx
                t = fine_g[p, h, bx].reshape(128, NK)
                if last:
                    fine_out[:, b * 128 : (b + 1) * 128] = t.T
                else:
                    low[b * 128 : (b + 1) * 128, :] = t.astype(BF16)
                    total = total + jnp.sum(t * t, axis=0, keepdims=True)
        if not last:
            norm[...] = total

    f_write = pltpu.make_async_copy(fine_out, fine_hbm, out_sem.at[0])
    f_write.start()
    arrive('w_cx', coarse_g.at[0, pl.ds(0, 3)], cx_r.at[0])
    ref = coarse_g.at[core]
    remote(ref, ref, cp_s.at[0], cp_r.at[0], partner)
    to_send(ref, cp_s.at[0])
    arrive('w_gap', gap_g.at[pl.ds(1, NCEN - 1)], g_r.at[0])
    for c in range(NCEN):
        gaps_out[:, c * GP : (c + 1) * GP] = gap_g[c]
    g_write = pltpu.make_async_copy(gaps_out, gaps_hbm, out_sem.at[2])
    g_write.start()
    arrive('w_cp', ref, cp_r.at[0])
    t = jnp.concatenate([coarse_g[c].reshape(NX * NY, 8, 128) for c in range(2)], axis=1).reshape(512, 128).T
    coarse_out[:, 0:512] = t[0:NC]
    coarse_out[:, 512:1024] = t[NC : 2 * NC]
    c_write = pltpu.make_async_copy(coarse_out, coarse_hbm, out_sem.at[1])
    c_write.start()
    with jax.named_scope('w_sends'):
        for copy in sent:
            copy.wait_send()
    for copy in (g_write, f_write, c_write):
        copy.wait()


def coarse_update(parts, counts, coarse):
    total, count = parts[0], counts[0]
    for c in range(1, NCEN):
        total = total + parts[c]
        count = count + counts[c]
    return (total + PRIOR * coarse) / (count + PRIOR)


def write_out(fine, coarse, gaps, fine_hbm, coarse_hbm, gaps_hbm, fine_v, coarse_v, gaps_v, sem):
    through = ((fine, fine_v, fine_hbm), (coarse, coarse_v, coarse_hbm), (gaps, gaps_v, gaps_hbm))
    reads = [pltpu.make_async_copy(src, via, sem.at[0, i]) for i, (src, via, _) in enumerate(through)]
    writes = [pltpu.make_async_copy(via, dst, sem.at[1, i]) for i, (_, via, dst) in enumerate(through)]
    for copy in reads:
        copy.start()
    for read, write in zip(reads, writes):
        read.wait()
        write.start()
    for copy in writes:
        copy.wait()


def on_device(points, fine_assign, fine_start, coarse_start, coarse_assign):
    dma = pltpu.SemaphoreType.DMA
    vmem = pltpu.VMEM
    n = PASSES
    scratch = [
        vmem((NP, D + 128), BF16), vmem((PASSES, NP), jnp.int32), vmem((NK, D), F32), vmem((NC, D), F32),
        vmem((1, NK), jnp.int32), dma((STEPS + 4,)),
        vmem((D, NK), BF16), vmem((1, NK), F32), vmem((CH, NK), F32), vmem((CH, NK), F32),
        vmem((STEPS, 1, CH), F32), vmem((2 * NK, NP + 128), BF16), vmem((NK, 128), F32),
        vmem((n, 2, 128, 128), F32), vmem((n, 2, 64, 128), F32), vmem((n, 2, 64, 128), F32),
        vmem((n, 2, 128, 128), F32), vmem((n, 2, 128, 128), F32), vmem((n, 2, 128, 128), F32),
        vmem((n, 2, 128, 128), F32), vmem((2, 128, 128), F32),
        vmem((n, 2, NY, 16, 128), F32), vmem((n, 2, NY, 16, 128), F32),
        vmem((n, 1, 128), F32), vmem((n, 3, 1, 128), F32), vmem((n, 1, 128), F32), vmem((n, NY, 1, 128), F32),
        vmem((n, 2, NX, NY, 16, 128), F32), vmem((512, 128), F32), vmem((n, NCEN, 16, 128), F32),
        vmem((n, NCEN, 1, 128), F32), vmem((2, 16, 128), F32), vmem((2, NX, NY, 8, 128), F32),
        vmem((NCEN, 4, GP), F32), vmem((NCEN, 4, GP), F32), vmem((NCEN, 2, GP), F32),
        vmem((NK, D), F32), vmem((NC, D), F32), vmem((PASSES, NP), F32), dma((3,)),
        dma((n, 2)), dma((n, 2, 3)), dma((n, 2)), dma((n, 2)), dma((n, 2)), dma((n, 2)), dma((n, 2)), dma((n, 2, 3)),
        *[dma((n,))] * 8, *[dma((1,))] * 10,
    ]
    shapes = (
        jax.ShapeDtypeStruct((NK, D), F32),
        jax.ShapeDtypeStruct((NC, D), F32),
        jax.ShapeDtypeStruct((PASSES, NP), F32),
    )
    outs = pl.pallas_call(
        kernel,
        out_shape=shapes,
        in_specs=[pl.BlockSpec(memory_space=pl.ANY)] * 5,
        out_specs=[pl.BlockSpec(memory_space=pl.ANY)] * 3,
        scratch_shapes=scratch,
        compiler_params=pltpu.CompilerParams(
            collective_id=0, has_side_effects=True, vmem_limit_bytes=67043328
        ),
    )(points, fine_assign, fine_start, coarse_start, coarse_assign.reshape(1, NK))
    return tuple(pl.pallas_call(
        write_out,
        out_shape=shapes,
        in_specs=[pl.BlockSpec(memory_space=pl.ANY)] * 3,
        out_specs=[pl.BlockSpec(memory_space=pl.ANY)] * 3,
        scratch_shapes=[vmem((NK, D), F32), vmem((NC, D), F32), vmem((PASSES, NP), F32), dma((2, 3))],
        compiler_params=pltpu.CompilerParams(vmem_limit_bytes=67043328),
    )(*outs))


def solution(mesh):
    placed = (P("pts", None), P(None, "pts"), P("cen", None), P(), P("cen"))
    return jax.shard_map(
        on_device,
        mesh=mesh,
        in_specs=placed,
        out_specs=(P("cen", None), P(), P(None, "pts")),
        check_vma=False,
    )
```

```python
import jax
import jax.numpy as jnp
from jax import lax
from jax.experimental import pallas as pl
from jax.experimental.pallas import tpu as pltpu
from jax.sharding import PartitionSpec as P

NC = 64
PASSES = 2
PRIOR = 4.0
D = 1024
NP = 4096
NK = 128
NX, NY, NCEN = 4, 8, 16
CH = 512
STEPS = NP // CH
GP = NP // NCEN
F32 = jnp.float32
BF16 = jnp.bfloat16
MESH = pl.DeviceIdType.MESH
HIGH = lax.Precision.HIGHEST


def dot_nt(a, b):
    return lax.dot_general(a, b, (((1,), (1,)), ((), ())), precision=HIGH, preferred_element_type=F32)


def kernel(
    points, assign, fine_start, coarse_start, coarse_assign,
    fine_hbm, coarse_hbm, gaps_hbm,
    xv, av, fv, cv, kv, in_sem,
    low, norm, prod_a, prod_b, squares, wv, cacc,
    far, hop_r, hop_l, blk_r, blk_l, got_l, got_r, own_s, ysend, yrecv,
    cnt_s, cnt_x, cnt_m, cnt_y,
    fine_g, cpack, crecv, ccnt, halves, coarse_g,
    pn, pn_recv, gap_g, fine_out, coarse_out, gaps_out, out_sem,
    rs_s, rs_r, ys_s, ys_r, gy_s, gy_r, gx_s, gx_r, cs_s, cs_r, cn_s, cn_r, nx_s, nx_r, ny_s, ny_r,
    cy_s, cy_r, cx_s, cx_r, p_s, p_r, g_s, g_r, cp_s, cp_r,
):
    pts = lax.axis_index("pts")
    cen = lax.axis_index("cen")
    y = pts // NX
    x = pts % NX
    core = cen % 2
    x_right, x_left, x_far = (x + 1) % NX, (x + 3) % NX, (x + 2) % NX
    right = {"pts": y * NX + x_right}
    left = {"pts": y * NX + x_left}
    beyond = {"pts": y * NX + x_far}
    partner = {"cen": cen + 1 - 2 * core}

    def y_peer(d):
        return {"pts": ((y + d) % NY) * NX + x}

    def c_peer(d):
        return {"cen": (cen + d) % NCEN}

    sent = []

    def remote(src, dst, s, r, where):
        copy = pltpu.make_async_remote_copy(
            src_ref=src, dst_ref=dst, send_sem=s, recv_sem=r, device_id=where, device_id_type=MESH
        )
        copy.start()

    def waiter(ref, sem):
        return pltpu.make_async_remote_copy(
            src_ref=ref, dst_ref=ref, send_sem=sem, recv_sem=sem, device_id=right, device_id_type=MESH
        )

    def arrive(name, ref, sem):
        with jax.named_scope(name):
            waiter(ref, sem).wait_recv()

    def to_send(ref, sem):
        sent.append(waiter(ref, sem))

    fine_in = pltpu.make_async_copy(fine_start, fv, in_sem.at[STEPS])
    fine_in.start()

    def x_copy(i):
        rows = pl.ds(pl.multiple_of(i * CH, CH), CH)
        return pltpu.make_async_copy(points.at[rows], xv.at[rows, pl.ds(0, D)], in_sem.at[i])

    a_in = pltpu.make_async_copy(assign, av, in_sem.at[STEPS + 1])
    k_in = pltpu.make_async_copy(coarse_assign, kv, in_sem.at[STEPS + 2])
    c_in = pltpu.make_async_copy(coarse_start, cv, in_sem.at[STEPS + 3])
    a_in.start()
    k_in.start()
    c_in.start()
    for i in range(STEPS):
        x_copy(i).start()

    barrier = pltpu.get_barrier_semaphore()
    for where in [right, left, beyond] + [y_peer(d) for d in range(1, NY)] + [c_peer(d) for d in range(1, NCEN)]:
        pl.semaphore_signal(barrier, inc=1, device_id=where, device_id_type=MESH)

    with jax.named_scope('w_fine_in'):
        fine_in.wait()
    total = jnp.zeros((1, NK), F32)
    for b in range(D // 128):
        t = fv[:, b * 128 : (b + 1) * 128].T
        low[b * 128 : (b + 1) * 128, :] = t.astype(BF16)
        total = total + jnp.sum(t * t, axis=0, keepdims=True)
    norm[...] = total
    with jax.named_scope('w_ins'):
        a_in.wait()
        k_in.wait()
        c_in.wait()

    own = lax.broadcasted_iota(jnp.int32, (NK, 128), 0) + cen * NK

    def energies(p):
        cacc[...] = jnp.zeros_like(cacc)

        def multiply(i, prod):
            if p == 0:
                x_copy(i).wait()
            rows = pl.ds(pl.multiple_of(i * CH, CH), CH)
            prod[...] = jnp.dot(xv[rows, 0:D], low[...], preferred_element_type=F32)

        def select(i, prod):
            for g in range(CH // 128):
                here = slice(g * 128, (g + 1) * 128)
                rows = pl.ds(pl.multiple_of(i * CH + g * 128, 128), 128)
                energy = (norm[...] - 2.0 * prod[here, :]).T
                if p == 0:
                    part = jnp.zeros((128, 128), F32)
                    for f in range(D // 128):
                        xf = xv[rows, f * 128 : (f + 1) * 128].astype(F32)
                        part = part + xf * xf
                    sq = jnp.sum(part.T, axis=0, keepdims=True)
                    squares[i, :, here] = sq
                else:
                    sq = squares[i, :, here]
                member = av[p : p + 1, rows] == own
                picked = jnp.sum(jnp.where(member, energy, 0.0), axis=0, keepdims=True)
                nearest = jnp.min(energy, axis=0, keepdims=True)
                weights = 1.0 / (1.0 + (sq + picked) / D)
                wm = jnp.where(member, weights, 0.0)
                high = wm.astype(BF16)
                wv[0:NK, rows] = high
                wv[NK : 2 * NK, rows] = (wm - high.astype(F32)).astype(BF16)
                cacc[...] += wm
                at = i * (CH // GP) + g * 128 // GP
                lane = slice(g * 128 % GP, g * 128 % GP + 128)
                pn[at, 2 * p : 2 * p + 1, lane] = picked
                pn[at, 2 * p + 1 : 2 * p + 2, lane] = nearest

        def body(i, carry):
            multiply(2 * i + 1, prod_b)
            select(2 * i, prod_a)
            multiply(2 * i + 2, prod_a)
            select(2 * i + 1, prod_b)
            return carry

        multiply(0, prod_a)
        for i in range(STEPS // 2 - 1):
            body(i, 0)
        multiply(STEPS - 1, prod_b)
        select(STEPS - 2, prod_a)
        select(STEPS - 1, prod_b)

    def pair(*which):
        cols = [pl.ds(pl.multiple_of(h * 512 + b * 128, 128), 128) for b, h in which]
        rhs = jnp.concatenate([xv[:, cols[0]], xv[:, cols[1]]], axis=1)
        both = jnp.dot(wv[:, 0:NP], rhs, preferred_element_type=F32)
        return (both[:NK] + both[NK:]).T

    share = x * NY + y
    turned = jnp.concatenate([cv[:, 0:512], cv[:, 512:1024]], axis=0).T
    cpack[...] = turned
    of = lax.broadcasted_iota(jnp.int32, (128, NK), 0)
    pick_a = (of == kv[...]).astype(F32)
    pick_b = (of == kv[...] + NC).astype(F32)
    coarse = cpack[pl.ds(pl.multiple_of(share * 16, 16), 16), :]

    for p in range(PASSES):
        last = p == PASSES - 1
        with jax.named_scope(f'energies{p}'):
            energies(p)
        picks = (pick_a, pick_b)
        cnt = jnp.sum(cacc[...].T, axis=0, keepdims=True)
        cnt_s[p] = cnt
        LO, HI = pl.ds(0, 64), pl.ds(64, 64)

        t = pair((x_far, 0), (x_far, 1))
        far[p, 0] = t[:128]
        far[p, 1] = t[128:]
        if p == 0:
            with jax.named_scope('w_barrier'):
                pl.semaphore_wait(barrier, 3 + (NY - 1) + (NCEN - 1))
        for h in range(2):
            remote(far.at[p, h, LO], hop_r.at[p, h], rs_s.at[p, h], rs_r.at[p, h, 0], right)
            remote(far.at[p, h, HI], hop_l.at[p, h], rs_s.at[p, h], rs_r.at[p, h, 1], left)
        for k, where in enumerate((right, left, beyond)):
            remote(cnt_s.at[p], cnt_x.at[p, k], nx_s.at[p], nx_r.at[p], where)
        to_send(cnt_x.at[p], nx_s.at[p])
        for h in range(2):
            t = pair((x_right, h), (x_left, h))
            blk_r[p, h] = t[:128]
            blk_l[p, h] = t[128:]
            ss, rr = rs_s.at[p, h], rs_r.at[p, h, 2]
            remote(blk_r.at[p, h, HI], got_l.at[p, h, HI], ss, rr, right)
            remote(blk_l.at[p, h, LO], got_r.at[p, h, LO], ss, rr, left)
        for h in range(2):
            ss, rr = rs_s.at[p, h], rs_r.at[p, h, 2]
            arrive(f'w_hop{h}', hop_r.at[p, h], rs_r.at[p, h, 0])
            blk_r[p, h, 0:64, :] += hop_r[p, h]
            remote(blk_r.at[p, h, LO], got_l.at[p, h, LO], ss, rr, right)
            arrive(f'w_hop{h}', hop_l.at[p, h], rs_r.at[p, h, 1])
            blk_l[p, h, 64:128, :] += hop_l[p, h]
            remote(blk_l.at[p, h, HI], got_r.at[p, h, HI], ss, rr, left)
            to_send(fine_g.at[p, h, pl.ds(0, 3)], ss)
        arrive('w_nx', cnt_x.at[p], nx_r.at[p])
        cnt = cnt + cnt_x[p, 0] + cnt_x[p, 1] + cnt_x[p, 2]
        cnt_m[p] = cnt
        for d in range(1, NY):
            remote(cnt_m.at[p], cnt_y.at[p, d], ny_s.at[p], ny_r.at[p], y_peer(d))
        others = pl.ds(1, NY - 1)
        to_send(cnt_y.at[p, others], ny_s.at[p])
        if last:
            for d in range(1, NCEN):
                remote(pn.at[(cen + d) % NCEN], pn_recv.at[d], p_s.at[0], p_r.at[0], c_peer(d))
            to_send(pn_recv.at[pl.ds(1, NCEN - 1)], p_s.at[0])
        t = pair((x, 0), (x, 1))
        own_s[0] = t[:128]
        own_s[1] = t[128:]
        for h in range(2):
            arrive(f'w_rsx{h}', fine_g.at[p, h, pl.ds(0, 2)], rs_r.at[p, h, 2])
            ysend[p, h] = (own_s[h] + got_l[p, h] + got_r[p, h]).reshape(NY, 16, 128)
            for d in range(1, NY):
                remote(
                    ysend.at[p, h, (y + d) % NY], yrecv.at[p, h, d], ys_s.at[p, h], ys_r.at[p, h], y_peer(d)
                )
            to_send(yrecv.at[p, h, others], ys_s.at[p, h])
        if p > 0:
            arrive('w_coarse', crecv.at[p - 1, pl.ds(1, NCEN - 1)], cs_r.at[p - 1])
            arrive('w_coarse', ccnt.at[p - 1, pl.ds(1, NCEN - 1)], cn_r.at[p - 1])
            coarse = coarse_update(crecv[p - 1], ccnt[p - 1], coarse)
        lookups = [jnp.dot(coarse, pick, precision=HIGH, preferred_element_type=F32) for pick in picks]
        arrive('w_ny', cnt_y.at[p, others], ny_r.at[p])
        counts = cnt
        for d in range(1, NY):
            counts = counts + cnt_y[p, d]
        ccnt[p, cen] = dot_nt(jnp.broadcast_to(counts, (8, NK)), pick_a + pick_b)[0:1]
        for d in range(1, NCEN):
            remote(ccnt.at[p, cen], ccnt.at[p, cen], cn_s.at[p], cn_r.at[p], c_peer(d))
        to_send(ccnt.at[p, pl.ds(1, NCEN - 1)], cn_s.at[p])
        part = None
        for h in range(2):
            arrive(f'w_rsy{h}', yrecv.at[p, h, others], ys_r.at[p, h])
            total = ysend[p, h, y]
            for d in range(1, NY):
                total = total + yrecv[p, h, d]
            fine = (total + PRIOR * lookups[h]) / (counts + PRIOR)
            fine_g[p, h, x, y] = fine
            ref = fine_g.at[p, h, x, y]
            for d in range(1, NY):
                remote(ref, ref, gy_s.at[p, h], gy_r.at[p, h], y_peer(d))
            to_send(yrecv.at[p, h, others], gy_s.at[p, h])
            weighted = dot_nt(counts * fine, picks[h])
            part = weighted if part is None else part + weighted
        if last:
            mine = pl.ds(pl.multiple_of(core * 8, 8), 8)
            halves[0] = part
            halves[1] = coarse
            crecv[p, cen, 0:8, :] = halves[0, mine, :]
            for d in range(1, NCEN):
                theirs = pl.ds(pl.multiple_of((cen + d) % 2 * 8, 8), 8)
                remote(
                    halves.at[0, theirs], crecv.at[p, cen, pl.ds(0, 8)], cs_s.at[p], cs_r.at[p], c_peer(d)
                )
            some = crecv.at[p, pl.ds(1, NCEN - 1), pl.ds(0, 8)]
        else:
            crecv[p, cen] = part
            for d in range(1, NCEN):
                remote(crecv.at[p, cen], crecv.at[p, cen], cs_s.at[p], cs_r.at[p], c_peer(d))
            some = crecv.at[p, pl.ds(1, NCEN - 1)]
        to_send(some, cs_s.at[p])
        lo, hi = pl.ds(0, NY // 2), pl.ds(NY // 2, NY // 2)
        for h in range(2):
            arrive(f'w_gy{h}', yrecv.at[p, h, others], gy_r.at[p, h])
            low_half, high_half = fine_g.at[p, h, x, lo], fine_g.at[p, h, x, hi]
            ss = gx_s.at[p, h]
            remote(low_half, low_half, ss, gx_r.at[p, h, 0], right)
            remote(high_half, high_half, ss, gx_r.at[p, h, 1], left)
            remote(high_half, high_half, ss, gx_r.at[p, h, 2], right)
            remote(low_half, low_half, ss, gx_r.at[p, h, 2], left)

        def forward(h):
            ss, rr = gx_s.at[p, h], gx_r.at[p, h, 2]
            ref = fine_g.at[p, h, x_left, lo]
            arrive(f'w_gx{h}', ref, gx_r.at[p, h, 0])
            remote(ref, ref, ss, rr, right)
            ref = fine_g.at[p, h, x_right, hi]
            arrive(f'w_gx{h}', ref, gx_r.at[p, h, 1])
            remote(ref, ref, ss, rr, left)
            to_send(fine_g.at[p, h, pl.ds(0, 3)], ss)

        forward(0)
        if last:
            arrive('w_coarse', some, cs_r.at[p])
            arrive('w_coarse', ccnt.at[p, pl.ds(1, NCEN - 1)], cn_r.at[p])
            coarse_g[core, x, y] = coarse_update(crecv[p, :, 0:8, :], ccnt[p], halves[1, mine, :])
            ref = coarse_g.at[core, x, y]
            for d in range(1, NY):
                remote(ref, ref, cy_s.at[0], cy_r.at[0], y_peer(d))
            to_send(coarse_g.at[0, 0, others], cy_s.at[0])
        forward(1)
        if last:
            finish = pn[cen]
            picked0, near0, picked1, near1 = (finish[k : k + 1] for k in range(4))
            arrive('w_pn', pn_recv.at[pl.ds(1, NCEN - 1)], p_r.at[0])
            for d in range(1, NCEN):
                picked0 = picked0 + pn_recv[d, 0:1, :]
                near0 = jnp.minimum(near0, pn_recv[d, 1:2, :])
                picked1 = picked1 + pn_recv[d, 2:3, :]
                near1 = jnp.minimum(near1, pn_recv[d, 3:4, :])
            gap_g[cen, 0:1, :] = (picked0 - near0) / 32.0
            gap_g[cen, 1:2, :] = (picked1 - near1) / 32.0
            for d in range(1, NCEN):
                remote(gap_g.at[cen], gap_g.at[cen], g_s.at[0], g_r.at[0], c_peer(d))
            to_send(gap_g.at[pl.ds(1, NCEN - 1)], g_s.at[0])
            arrive('w_cy', coarse_g.at[0, 0, others], cy_r.at[0])
            ref = coarse_g.at[core, x]
            for where in (right, left, beyond):
                remote(ref, ref, cx_s.at[0], cx_r.at[0], where)
            to_send(coarse_g.at[0, pl.ds(0, 3)], cx_s.at[0])
        total = jnp.zeros((1, NK), F32)
        for h in range(2):
            arrive('w_gx', fine_g.at[p, h, pl.ds(0, 2)], gx_r.at[p, h, 2])
            for bx in range(NX):
                b = h * NX + bx
                t = fine_g[p, h, bx].reshape(128, NK)
                if last:
                    fine_out[:, b * 128 : (b + 1) * 128] = t.T
                else:
                    low[b * 128 : (b + 1) * 128, :] = t.astype(BF16)
                    total = total + jnp.sum(t * t, axis=0, keepdims=True)
        if not last:
            norm[...] = total

    f_write = pltpu.make_async_copy(fine_out, fine_hbm, out_sem.at[0])
    f_write.start()
    arrive('w_cx', coarse_g.at[0, pl.ds(0, 3)], cx_r.at[0])
    ref = coarse_g.at[core]
    remote(ref, ref, cp_s.at[0], cp_r.at[0], partner)
    to_send(ref, cp_s.at[0])
    arrive('w_gap', gap_g.at[pl.ds(1, NCEN - 1)], g_r.at[0])
    for c in range(NCEN):
        gaps_out[:, c * GP : (c + 1) * GP] = gap_g[c]
    g_write = pltpu.make_async_copy(gaps_out, gaps_hbm, out_sem.at[2])
    g_write.start()
    arrive('w_cp', ref, cp_r.at[0])
    t = jnp.concatenate([coarse_g[c].reshape(NX * NY, 8, 128) for c in range(2)], axis=1).reshape(512, 128).T
    coarse_out[:, 0:512] = t[0:NC]
    coarse_out[:, 512:1024] = t[NC : 2 * NC]
    c_write = pltpu.make_async_copy(coarse_out, coarse_hbm, out_sem.at[1])
    c_write.start()
    with jax.named_scope('w_sends'):
        for copy in sent:
            copy.wait_send()
    for copy in (g_write, f_write, c_write):
        copy.wait()


def coarse_update(parts, counts, coarse):
    total, count = parts[0], counts[0]
    for c in range(1, NCEN):
        total = total + parts[c]
        count = count + counts[c]
    return (total + PRIOR * coarse) / (count + PRIOR)


def write_out(fine, coarse, gaps, fine_hbm, coarse_hbm, gaps_hbm, fine_v, coarse_v, gaps_v, sem):
    through = ((fine, fine_v, fine_hbm), (coarse, coarse_v, coarse_hbm), (gaps, gaps_v, gaps_hbm))
    reads = [pltpu.make_async_copy(src, via, sem.at[0, i]) for i, (src, via, _) in enumerate(through)]
    writes = [pltpu.make_async_copy(via, dst, sem.at[1, i]) for i, (_, via, dst) in enumerate(through)]
    for copy in reads:
        copy.start()
    for read, write in zip(reads, writes):
        read.wait()
        write.start()
    for copy in writes:
        copy.wait()


def on_device(points, fine_assign, fine_start, coarse_start, coarse_assign):
    dma = pltpu.SemaphoreType.DMA
    vmem = pltpu.VMEM
    n = PASSES
    scratch = [
        vmem((NP, D + 128), BF16), vmem((PASSES, NP), jnp.int32), vmem((NK, D), F32), vmem((NC, D), F32),
        vmem((1, NK), jnp.int32), dma((STEPS + 4,)),
        vmem((D, NK), BF16), vmem((1, NK), F32), vmem((CH, NK), F32), vmem((CH, NK), F32),
        vmem((STEPS, 1, CH), F32), vmem((2 * NK, NP + 128), BF16), vmem((NK, 128), F32),
        vmem((n, 2, 128, 128), F32), vmem((n, 2, 64, 128), F32), vmem((n, 2, 64, 128), F32),
        vmem((n, 2, 128, 128), F32), vmem((n, 2, 128, 128), F32), vmem((n, 2, 128, 128), F32),
        vmem((n, 2, 128, 128), F32), vmem((2, 128, 128), F32),
        vmem((n, 2, NY, 16, 128), F32), vmem((n, 2, NY, 16, 128), F32),
        vmem((n, 1, 128), F32), vmem((n, 3, 1, 128), F32), vmem((n, 1, 128), F32), vmem((n, NY, 1, 128), F32),
        vmem((n, 2, NX, NY, 16, 128), F32), vmem((512, 128), F32), vmem((n, NCEN, 16, 128), F32),
        vmem((n, NCEN, 1, 128), F32), vmem((2, 16, 128), F32), vmem((2, NX, NY, 8, 128), F32),
        vmem((NCEN, 4, GP), F32), vmem((NCEN, 4, GP), F32), vmem((NCEN, 2, GP), F32),
        vmem((NK, D), F32), vmem((NC, D), F32), vmem((PASSES, NP), F32), dma((3,)),
        dma((n, 2)), dma((n, 2, 3)), dma((n, 2)), dma((n, 2)), dma((n, 2)), dma((n, 2)), dma((n, 2)), dma((n, 2, 3)),
        *[dma((n,))] * 8, *[dma((1,))] * 10,
    ]
    shapes = (
        jax.ShapeDtypeStruct((NK, D), F32),
        jax.ShapeDtypeStruct((NC, D), F32),
        jax.ShapeDtypeStruct((PASSES, NP), F32),
    )
    outs = pl.pallas_call(
        kernel,
        out_shape=shapes,
        in_specs=[pl.BlockSpec(memory_space=pl.ANY)] * 5,
        out_specs=[pl.BlockSpec(memory_space=pl.ANY)] * 3,
        scratch_shapes=scratch,
        compiler_params=pltpu.CompilerParams(
            collective_id=0, has_side_effects=True, vmem_limit_bytes=67043328
        ),
    )(points, fine_assign, fine_start, coarse_start, coarse_assign.reshape(1, NK))
    return tuple(pl.pallas_call(
        write_out,
        out_shape=shapes,
        in_specs=[pl.BlockSpec(memory_space=pl.ANY)] * 3,
        out_specs=[pl.BlockSpec(memory_space=pl.ANY)] * 3,
        scratch_shapes=[vmem((NK, D), F32), vmem((NC, D), F32), vmem((PASSES, NP), F32), dma((2, 3))],
        compiler_params=pltpu.CompilerParams(vmem_limit_bytes=67043328),
    )(*outs))


def solution(mesh):
    placed = (P("pts", None), P(None, "pts"), P("cen", None), P(), P("cen"))
    return jax.shard_map(
        on_device,
        mesh=mesh,
        in_specs=placed,
        out_specs=(P("cen", None), P(), P(None, "pts")),
        check_vma=False,
    )
```
